256 devices in a mesh: rep: 2 (over core), dp: 128 (over x, y, z).
Axes of the slice: x: 4, y: 4, z: 8, core: 2. Of those that a mesh axis runs over, the one named last changes fastest.
Arguments:
- x: bfloat16 [256, 2048, 896], P(('rep', 'dp')), parts along dimension 0
- dy: bfloat16 [256, 2048, 896], P(('rep', 'dp')), parts along dimension 0
- wq: bfloat16 [1, 896, 896], replicated
- wk: bfloat16 [1, 896, 128], replicated
- wv: bfloat16 [1, 896, 128], replicated
- wo: bfloat16 [1, 896, 896], replicated
- w_gate: bfloat16 [1, 896, 2560], replicated
- w_up: bfloat16 [1, 896, 2560], replicated
- w_down: bfloat16 [1, 2560, 896], replicated
- m_wq: float32 [1, 896, 896], replicated
- m_wk: float32 [1, 896, 128], replicated
- m_wv: float32 [1, 896, 128], replicated
- m_wo: float32 [1, 896, 896], replicated
- m_w_gate: float32 [1, 896, 2560], replicated
- m_w_up: float32 [1, 896, 2560], replicated
- m_w_down: float32 [1, 2560, 896], replicated
- v_wq: float32 [1, 896, 896], replicated
- v_wk: float32 [1, 896, 128], replicated
- v_wv: float32 [1, 896, 128], replicated
- v_wo: float32 [1, 896, 896], replicated
- v_w_gate: float32 [1, 896, 2560], replicated
- v_w_up: float32 [1, 896, 2560], replicated
- v_w_down: float32 [1, 2560, 896], replicated
Outputs:
- output 1: bfloat16 [2, 896, 896], P('rep'), parts along dimension 0
- output 2: bfloat16 [2, 896, 128], P('rep'), parts along dimension 0
- output 3: bfloat16 [2, 896, 128], P('rep'), parts along dimension 0
- output 4: bfloat16 [2, 896, 896], P('rep'), parts along dimension 0
- output 5: bfloat16 [2, 896, 2560], P('rep'), parts along dimension 0
- output 6: bfloat16 [2, 896, 2560], P('rep'), parts along dimension 0
- output 7: bfloat16 [2, 2560, 896], P('rep'), parts along dimension 0
- output 8: float32 [2, 896, 896], P('rep'), parts along dimension 0
- output 9: float32 [2, 896, 128], P('rep'), parts along dimension 0
- output 10: float32 [2, 896, 128], P('rep'), parts along dimension 0
- output 11: float32 [2, 896, 896], P('rep'), parts along dimension 0
- output 12: float32 [2, 896, 2560], P('rep'), parts along dimension 0
- output 13: float32 [2, 896, 2560], P('rep'), parts along dimension 0
- output 14: float32 [2, 2560, 896], P('rep'), parts along dimension 0
- output 15: float32 [2, 896, 896], P('rep'), parts along dimension 0
- output 16: float32 [2, 896, 128], P('rep'), parts along dimension 0
- output 17: float32 [2, 896, 128], P('rep'), parts along dimension 0
- output 18: float32 [2, 896, 896], P('rep'), parts along dimension 0
- output 19: float32 [2, 896, 2560], P('rep'), parts along dimension 0
- output 20: float32 [2, 896, 2560], P('rep'), parts along dimension 0
- output 21: float32 [2, 2560, 896], P('rep'), parts along dimension 0
There are 2 independent parts. The reference program is written for one: setup_inputs(seed, part) draws one part's arguments, and reference() takes and returns one part's arrays. A program takes and returns all parts, laid end to end along the dimension named above; an argument that names none is the same for every part.
All inputs are finite; a program needn't handle non-finite values.
Results may differ from the reference program's by a relative error of at most 0.024.
Values are sent between devices in bfloat16 or wider.
A program may use at most 768 MiB of HBM per device.

```python
import jax
import jax.numpy as jnp
from jax import lax

SEQUENCES = 128
TOKENS = 2048
D = 896
HEADS = 7
KV_HEADS = 1
HEAD = 128
FF = 2560
LAYERS = 1
THETA = 10000
NAMES = ("wq", "wk", "wv", "wo", "w_gate", "w_up", "w_down")
SHAPES = {
    "wq": (LAYERS, D, HEADS * HEAD),
    "wk": (LAYERS, D, KV_HEADS * HEAD),
    "wv": (LAYERS, D, KV_HEADS * HEAD),
    "wo": (LAYERS, HEADS * HEAD, D),
    "w_gate": (LAYERS, D, FF),
    "w_up": (LAYERS, D, FF),
    "w_down": (LAYERS, FF, D),
}


def bump(key, n, height):
    away = (jnp.arange(n, dtype=jnp.int32) - jax.random.randint(key, (), 0, n, jnp.int32)) % n
    return jnp.where(away < n // 8, height, 1.0)


def together(key, own, strength):
    shared = jax.random.normal(key, own.shape[1:], jnp.float32)
    return (own + strength * shared) * lax.rsqrt(1 + strength * strength)


def setup_inputs(seed: int = 0, part: int = 0) -> dict:
    kx, kdy, ka, kb, kz, kf, kh, kl, *keys = jax.random.split(jax.random.key(seed), 8 + 3 * len(NAMES))
    kx, kdy, ka, kb = (jax.random.fold_in(k, part) for k in (kx, kdy, ka, kb))
    kw, km, kv = (keys[i::3] for i in range(3))
    shape = (SEQUENCES, TOKENS, D)
    much_x, much_dy = jax.random.uniform(kz, (2,), jnp.float32, 0.0, 1.0)
    loud = 2.0 ** jax.random.uniform(jax.random.fold_in(kz, 1), (), jnp.float32, -1.0, 2.0)
    layers = 2.0 ** jax.random.uniform(kl, (LAYERS, 1, 1), jnp.float32, -1.0, 1.0)
    times = {"wq": 1.0, "wk": 1.0, "wv": 2.0, "wo": layers, "w_gate": 1.0, "w_up": bump(kh, FF, 4.0), "w_down": layers}
    x = together(ka, jax.random.normal(kx, shape, jnp.float32), much_x) * bump(kf, D, 4.0)
    dy = together(kb, jax.random.normal(kdy, shape, jnp.float32), much_dy)
    drawn = {"x": x.astype(jnp.bfloat16), "dy": (loud * dy * (SEQUENCES * TOKENS) ** -0.5).astype(jnp.bfloat16)}
    for key, name in zip(kw, NAMES, strict=True):
        drawn[name] = (jax.random.normal(key, SHAPES[name], jnp.float32) * SHAPES[name][1] ** -0.5 * times[name]).astype(jnp.bfloat16)
    for key, name in zip(km, NAMES, strict=True):
        drawn[f"m_{name}"] = 0.1 * jax.random.normal(key, SHAPES[name], jnp.float32)
    for key, name in zip(kv, NAMES, strict=True):
        drawn[f"v_{name}"] = jax.random.uniform(key, SHAPES[name], jnp.float32, 0.02, 0.06)
    return drawn


def matmul(a, w):
    return jnp.dot(a, w, preferred_element_type=jnp.float32).astype(jnp.bfloat16)


def normed(h):
    wide = h.astype(jnp.float32)
    scale = lax.rsqrt(jnp.mean(wide**2, -1, keepdims=True) + 1e-6)
    return (wide * scale).astype(jnp.bfloat16)


def turned(t, theta):
    half = t.shape[-1] // 2
    angle = jnp.arange(t.shape[0], dtype=jnp.float32)[:, None] * theta ** (-jnp.arange(half, dtype=jnp.float32) / half)
    cos, sin = jnp.cos(angle)[:, None], jnp.sin(angle)[:, None]
    a, b = t[..., :half].astype(jnp.float32), t[..., half:].astype(jnp.float32)
    return jnp.concatenate([a * cos - b * sin, b * cos + a * sin], -1).astype(jnp.bfloat16)


def seen_by(q, k, v):
    tokens, kv = q.shape[0], k.shape[1]
    q = q.reshape(tokens, kv, -1, q.shape[-1])
    scores = jnp.einsum("tgsd,ugd->gstu", q.astype(jnp.float32), k.astype(jnp.float32)) * q.shape[-1] ** -0.5
    place = jnp.arange(tokens)
    weights = jax.nn.softmax(jnp.where(place[:, None] >= place, scores, -jnp.inf), -1).astype(jnp.bfloat16)
    return jnp.einsum("gstu,ugd->tgsd", weights.astype(jnp.float32), v.astype(jnp.float32)).astype(jnp.bfloat16).reshape(tokens, -1)


def layer(h, w):
    a = normed(h)
    q, k = (turned(matmul(a, w[name]).reshape(h.shape[0], -1, HEAD), THETA) for name in ("wq", "wk"))
    h = h + matmul(seen_by(q, k, matmul(a, w["wv"]).reshape(h.shape[0], -1, HEAD)), w["wo"])
    b = normed(h)
    gate = jnp.dot(b, w["w_gate"], preferred_element_type=jnp.float32)
    up = jnp.dot(b, w["w_up"], preferred_element_type=jnp.float32)
    return h + matmul((jax.nn.silu(gate) * up).astype(jnp.bfloat16), w["w_down"])


def adamw(w, m, v, g):
    m = 0.9 * m + 0.1 * g
    v = 0.95 * v + 0.05 * g * g
    step = m * lax.rsqrt(v + 1e-8) + 0.1 * w
    return (w - 0.02 * step).astype(jnp.bfloat16), m, v


def clipped(gradients, sum_of_squares, count):
    factor = jnp.minimum(1.0, 0.5 * lax.rsqrt(sum_of_squares / count + 1e-30))
    return [g * factor for g in gradients]


def stack(weights, h):
    return lax.scan(lambda h, w: (layer(h, w), None), h, weights)[0]


def reference(x, dy, wq, wk, wv, wo, w_gate, w_up, w_down, m_wq, m_wk, m_wv, m_wo, m_w_gate, m_w_up, m_w_down, v_wq, v_wk, v_wv, v_wo, v_w_gate, v_w_up, v_w_down):
    weights = dict(zip(NAMES, (wq, wk, wv, wo, w_gate, w_up, w_down), strict=True))

    def take(so_far, sequence):
        h, by_y = sequence
        _, back = jax.vjp(stack, weights, h)
        by_weights, by_h = back(by_y)
        return jax.tree.map(lambda total, term: total + term.astype(jnp.float32), so_far, by_weights), by_h

    none_yet = {name: jnp.zeros(w.shape, jnp.float32) for name, w in weights.items()}
    by_weights, by_x = lax.scan(take, none_yet, (x, dy))
    gradients = [by_weights[name].astype(jnp.bfloat16).astype(jnp.float32) for name in NAMES]
    gradients = clipped(gradients, sum(jnp.sum(g * g) for g in gradients), sum(g.size for g in gradients))
    first = (m_wq, m_wk, m_wv, m_wo, m_w_gate, m_w_up, m_w_down)
    second = (v_wq, v_wk, v_wv, v_wo, v_w_gate, v_w_up, v_w_down)
    new = [adamw(weights[name].astype(jnp.float32), m, v, g) for name, m, v, g in zip(NAMES, first, second, gradients, strict=True)]
    return tuple(one[which] for which in range(3) for one in new)
```

```python
import functools

import jax
import jax.numpy as jnp
import numpy as np
from jax import lax
from jax.experimental import pallas as pl
from jax.experimental.pallas import tpu as pltpu
from jax.sharding import PartitionSpec as P

BF, F32 = jnp.bfloat16, jnp.float32
MESH = pl.DeviceIdType.MESH
ANY = pl.BlockSpec(memory_space=pl.ANY)
LANE, HALF = 128, 64
D, HEADS, FF, TOKENS = 896, 7, 2560, 2048
THETA = 10000
TILE = 512
CHUNKS = TOKENS // LANE
FLAT = HEADS * TOKENS
STEP = 256
MLP = FF // STEP
TINY = 1e-6
SCALE = LANE**-0.5
E = SCALE * 1.4426950408889634
NEG = -1e30
MIB = 2**20


def dot(a, b, ca=1, cb=0):
    return lax.dot_general(a, b, (((ca,), (cb,)), ((), ())), preferred_element_type=F32)


def normed(h):
    wide = h.astype(F32)
    scale = lax.rsqrt(jnp.mean(wide * wide, -1, keepdims=True) + TINY)
    return (wide * scale).astype(BF), scale


def dot_t(a, b):
    return dot(a, b, 1, 1)


def columns(a):
    return [a[:, n : n + LANE] for n in range(0, a.shape[1], LANE)]


def rows(start, size):
    return pl.ds(start if isinstance(start, int) else pl.multiple_of(start, size), size)


def tables():
    angle = np.arange(TOKENS, dtype=np.float64)[:, None] * THETA ** (-np.arange(HALF, dtype=np.float64) / HALF)
    cos, sin = np.cos(angle), np.sin(angle)
    return jnp.asarray(np.concatenate([cos, cos], 1), F32), jnp.asarray(np.concatenate([-sin, sin], 1), F32)


def project_kernel(x_ref, cos_ref, sin_ref, wq_ref, wk_ref, wv_ref, q_ref, k_ref, v_ref, at_ref):
    a, _ = normed(x_ref[0])
    for n, part in enumerate(columns(a.T)):
        at_ref[n] = part

    def turned(t):
        t = t.astype(BF).astype(F32)
        return (t * cos_ref[...] + pltpu.roll(t, HALF, 1) * sin_ref[...]).astype(BF)

    for n, part in enumerate(columns(dot(a, wq_ref[0]))):
        q_ref[n] = turned(part)
    k_ref[...] = turned(dot(a, wk_ref[0]))
    v_ref[...] = dot(a, wv_ref[0]).astype(BF)


def cost(flops, megabytes):
    return pl.CostEstimate(flops=flops, bytes_accessed=megabytes * MIB, transcendentals=0)


def like(*shape, dtype=BF):
    return jax.ShapeDtypeStruct(shape, dtype)


def whole(shape):
    return pl.BlockSpec(shape, lambda i: (0,) * len(shape))


TILES = pl.BlockSpec((1, TILE, D), lambda i: (0, i, 0))
NARROW = pl.BlockSpec((TILE, LANE), lambda i: (i, 0))
SPLIT = pl.BlockSpec((HEADS, TILE, LANE), lambda i: (0, i, 0))
TURNED = pl.BlockSpec((TILE // LANE, D, LANE), lambda i: (i, 0, 0))
ROOM = pltpu.CompilerParams(vmem_limit_bytes=48 * MIB)
STEPS = (TOKENS // TILE,)


def project(x, wq, wk, wv, cos, sin):
    return pl.pallas_call(
        project_kernel,
        grid=STEPS,
        in_specs=[TILES, NARROW, NARROW, whole((1, D, D)), whole((1, D, LANE)), whole((1, D, LANE))],
        out_specs=[SPLIT, NARROW, NARROW, TURNED],
        out_shape=[like(HEADS, TOKENS, LANE), like(TOKENS, LANE), like(TOKENS, LANE), like(CHUNKS, D, LANE)],
        compiler_params=ROOM,
        cost_estimate=cost(2 * TOKENS * D * (D + 2 * LANE), 12),
    )(x, cos, sin, wq, wk, wv)


def attend_kernel(q_ref, k_ref, v_ref, o_ref, lse_ref, top_s, mix_s):
    iq = pl.program_id(0)
    top_s[...] = jnp.full_like(top_s, NEG)
    mix_s[...] = jnp.zeros_like(mix_s)
    ones = jnp.ones((8, TILE), BF)

    def block(j, masked):
        here = rows(j * TILE, TILE)
        scores = [dot_t(k_ref[here, :], q_ref[n]) for n in range(HEADS)]
        if masked:
            gap = lax.broadcasted_iota(jnp.int32, (TILE, TILE), 1) - lax.broadcasted_iota(jnp.int32, (TILE, TILE), 0)
        weights, keeps = [], []
        for n, s in enumerate(scores):
            if masked:
                s = jnp.where(gap >= 0, s, 2 * NEG)
            old = top_s[n : n + 1, :]
            top = jnp.maximum(old, s.max(axis=0, keepdims=True))
            top_s[n : n + 1, :] = top
            weights.append(jnp.exp2((s - top) * E).astype(BF))
            keeps.append(jnp.exp2((old - top) * E))
        values = jnp.concatenate([v_ref[here, :].T, ones], axis=0)
        for n in range(HEADS):
            mix_s[n] = mix_s[n] * keeps[n] + dot(values, weights[n])

    lax.fori_loop(0, iq, lambda j, _: block(j, False), None)
    block(iq, True)
    for n in range(HEADS):
        total = mix_s[n, LANE : LANE + 1, :]
        o_ref[n] = (mix_s[n, :LANE, :] * (1 / total)).T.astype(BF)
        lse_ref[n : n + 1, :] = top_s[n : n + 1, :] * SCALE + jnp.log(total)


def attend(q, k, v):
    return pl.pallas_call(
        attend_kernel,
        grid=STEPS,
        in_specs=[SPLIT, whole((TOKENS, LANE)), whole((TOKENS, LANE))],
        out_specs=[SPLIT, pl.BlockSpec((HEADS, TILE), lambda i: (0, i))],
        out_shape=[like(HEADS, TOKENS, LANE), like(HEADS, TOKENS, dtype=F32)],
        scratch_shapes=[pltpu.VMEM((HEADS, TILE), F32), pltpu.VMEM((HEADS, LANE + 8, TILE), F32)],
        compiler_params=ROOM,
        cost_estimate=cost(4 * HEADS * TOKENS * TOKENS * LANE, 8),
    )(q, k, v)


def middle_kernel(att_ref, x_ref, dy_ref, wo_ref, h_ref, b_ref, bt_ref, dyt_ref, attt_ref):
    att = jnp.concatenate([att_ref[n] for n in range(HEADS)], 1)
    h = (x_ref[0].astype(F32) + dot(att, wo_ref[0]).astype(BF).astype(F32)).astype(BF)
    h_ref[...] = h
    b, _ = normed(h)
    for n, part in enumerate(columns(b)):
        b_ref[n] = part
    for ref, a in ((bt_ref, b), (dyt_ref, dy_ref[0]), (attt_ref, att)):
        for n, part in enumerate(columns(a.T)):
            ref[n] = part


def middle(att, x, dy, wo):
    return pl.pallas_call(
        middle_kernel,
        grid=STEPS,
        in_specs=[SPLIT, TILES, TILES, whole((1, D, D))],
        out_specs=[pl.BlockSpec((TILE, D), lambda i: (i, 0)), SPLIT, TURNED, TURNED, TURNED],
        out_shape=[like(TOKENS, D), like(HEADS, TOKENS, LANE)] + [like(CHUNKS, D, LANE)] * 3,
        compiler_params=ROOM,
        cost_estimate=cost(2 * TOKENS * D * D, 28),
    )(att, x, dy, wo)


ROWS = 1792
SIZE = {"x": 4, "y": 4, "z": 8}
STRIDE = {"x": 32, "y": 8, "z": 1}
COLOURS = ("xyz", "yxz", "zxy")
GS = 4


def up(n, m):
    return -(-n // m) * m


FIRST, SECOND, THIRD = range(3)
WAYS = 0, 1
UP, DOWN = WAYS


def place(me, dim):
    return (me // STRIDE[dim]) % SIZE[dim]


def turn(way):
    return 1 - 2 * way


def near(first, size):
    return pl.ds(pl.multiple_of(first, 16), size)


def start(copies):
    for copy in copies:
        copy.start()


def wait(copies):
    for copy in copies:
        copy.wait()


class Colour:
    def __init__(self, dims):
        self.dims = dims
        self.n = self.n1, self.n2, self.n3 = [SIZE[d] for d in dims]
        self.u1 = ROWS // self.n1
        self.pad1 = up(self.u1, self.n2 * 16)
        self.u2 = self.pad1 // self.n2
        self.pad2 = up(self.u2, self.n3 * 16)
        self.u3 = self.pad2 // self.n3
        self.h1, self.h2 = self.n1 // 2, self.n2 // 2
        self.half1 = up(self.u1 // 2, 16)
        self.half2 = up(self.u2 // 2, 16)
        self.slots = 3 + self.h1 // 2
        self.last = 2 * self.h1 + 6

    def scratch(self):
        def twice(*shape, dtype=BF):
            return pltpu.VMEM((2, *shape, LANE), dtype)

        def sems(*shape):
            return pltpu.SemaphoreType.DMA((2, 2, *shape))

        r1, r2 = self.half1 + (self.h1 - 1) * self.u1, self.half2 + (self.h2 - 1) * self.u2
        ways = len(WAYS)
        return [
            twice(ways, r1),
            twice(self.pad1, dtype=F32),
            twice(ways + 1, self.u2),
            twice(ways, r2),
            twice(self.pad2, dtype=F32),
            twice(self.pad2),
            twice(self.n3, self.u3),
            twice(self.pad2),
            pltpu.VMEM((3, self.pad1, LANE), BF),
            pltpu.VMEM((self.slots, ROWS, LANE), BF),
            sems(ways, self.h1),
            sems(ways, self.h2),
            sems(self.n3),
            sems(self.n3),
            sems(ways, self.h2),
            sems(ways, self.h1),
            pltpu.SemaphoreType.DMA((2,)),
        ]

    def bind(self, refs, g_ref, number, me, out):
        (self.r1, self.s1, self.t2, self.r2, self.s2, self.t3, self.r3, self.o3, self.o2, self.o,
         self.q1, self.q2, self.q3, self.a3, self.a2, self.a1, self.qo) = refs
        self.g, self.number, self.out, self.me = g_ref, number, out, me
        self.p = self.p1, self.p2, self.p3 = [place(me, d) for d in self.dims]

    def peer(self, k, off):
        d, n = self.dims[k], self.n[k]
        return {"dp": self.me + (lax.rem(self.p[k] + off + n, n) - self.p[k]) * STRIDE[d]}

    def zero(self):
        for ref in (self.s1, self.s2):
            ref[...] = jnp.zeros_like(ref)

    def _ring(self, k, src, dst, sems, par, way, step):
        return pltpu.make_async_remote_copy(src, dst, sems.at[0, par, way, step], sems.at[1, par, way, step],
                                            device_id=self.peer(k, turn(way)), device_id_type=MESH)

    def _span(self, halved, t, way, u, half):
        first, size = (0, u) if not halved else (0, half) if way == UP else (half, u - half)
        return first, size, max(half + (t - 2) * u, 0) if t > 1 else 0

    def rs1(self, t, way, gs, par):
        n, u = self.n1, self.u1
        dest = lax.rem(self.p1 + turn(way) * (self.h1 + 1 - t) + n, n)
        first, size, at = self._span(t == 1, t, way, u, self.half1)
        return self._ring(FIRST, self.g.at[gs, self.number, near(dest * u + first, size)], self.r1.at[par, way, pl.ds(at, size)], self.q1, par, way, t - 1)

    def rs2(self, t, way, par):
        first, size, at = self._span(t == 1, t, way, self.u2, self.half2)
        return self._ring(SECOND, self.t2.at[par, len(WAYS) if t == 1 else way, pl.ds(first, size)], self.r2.at[par, way, pl.ds(at, size)], self.q2, par, way, t - 1)

    def rs3(self, par):
        n, u = self.n3, self.u3
        return [pltpu.make_async_remote_copy(self.t3.at[par, near(lax.rem(self.p3 + off, n) * u, u)], self.r3.at[par, off], self.q3.at[0, par, off],
                                             self.q3.at[1, par, off], device_id=self.peer(THIRD, off), device_id_type=MESH) for off in range(1, n)]

    def ag3(self, par):
        mine = self.o3.at[par, near(self.p3 * self.u3, self.u3)]
        return [pltpu.make_async_remote_copy(mine, mine, self.a3.at[0, par, off], self.a3.at[1, par, off], device_id=self.peer(THIRD, off),
                                             device_id_type=MESH) for off in range(1, self.n3)]

    def _ag(self, k, t, way, par, ref, u, half, h, sems):
        n = self.n[k]
        piece = lax.rem(self.p[k] - turn(way) * (t - 1) + n, n)
        first, size, _ = self._span(t == h, t, way, u, half)
        here = ref.at[near(piece * u + first, size)]
        return self._ring(k, here, here, sems, par, way, t - 1)

    def ag2(self, t, par, third):
        return [self._ag(SECOND, t, way, par, self.o2.at[third], self.u2, self.half2, self.h2, self.a2) for way in WAYS]

    def ag1(self, t, par, os):
        return [self._ag(FIRST, t, way, par, self.o.at[os], self.u1, self.half1, self.h1, self.a1) for way in WAYS]

    def output(self, c, os):
        return pltpu.make_async_copy(self.o.at[os], self.out.at[c, self.number], self.qo.at[lax.rem(c, 2)])

    def event(self, e, c, squares=None):
        par, third, gs, os = lax.rem(c, 2), lax.rem(c, 3), lax.rem(c, GS), lax.rem(c, self.slots)
        h1, f32, bf = self.h1, F32, BF
        if e <= h1:
            if e > 0:
                wait(self.rs1(e, way, gs, par) for way in WAYS)
            if e < h1:
                for way in WAYS:
                    if e > 0:
                        n, h, u, half = self.n1, self.h1, self.u1, self.half1
                        first, many, came = self._span(e == 1, e, way, u, half)
                        dest = lax.rem(self.p1 + turn(way) * (h - e) + n, n)
                        into = near(dest * u + first, many)
                        self.g[gs, self.number, into, :] = (self.g[gs, self.number, into, :].astype(f32) + self.r1[par, way, came:came + many, :].astype(f32)).astype(bf)
                    self.rs1(e + 1, way, gs, par).start()
                return
            u = self.u1
            _, _, at = self._span(False, h1, UP, u, self.half1)
            self.s1[par, :u, :] = (self.g[gs, self.number, near(self.p1 * u, u), :].astype(f32) + self.r1[par, 0, at:at + u, :].astype(f32)
                                   + self.r1[par, 1, at:at + u, :].astype(f32))
            opposite = lax.rem(self.p2 + 2, 4)
            self.t2[par, 2] = self.s1[par, near(opposite * self.u2, self.u2), :].astype(bf)
            start(self.rs2(1, way, par) for way in WAYS)
        elif e == h1 + 1:
            wait(self.rs2(1, way, par) for way in WAYS)
            for way in WAYS:
                dest = lax.rem(self.p2 + turn(way) + 4, 4)
                base, half = dest * self.u2, self.half2
                lo = self.s1[par, near(base, half), :]
                hi = self.s1[par, near(base + half, self.u2 - half), :]
                if way == UP:
                    lo = lo + self.r2[par, 0, :half, :].astype(f32)
                else:
                    hi = hi + self.r2[par, 1, :self.u2 - half, :].astype(f32)
                self.t2[par, way, :half, :] = lo.astype(bf)
                self.t2[par, way, half:, :] = hi.astype(bf)
                self.rs2(2, way, par).start()
        elif e == h1 + 2:
            wait(self.rs2(2, way, par) for way in WAYS)
            u, at = self.u2, self.half2
            self.s2[par, :u, :] = (self.s1[par, near(self.p2 * u, u), :] + self.r2[par, 0, at:at + u, :].astype(f32)
                                   + self.r2[par, 1, at:at + u, :].astype(f32))
            self.t3[par] = self.s2[par].astype(bf)
            start(self.rs3(par))
        elif e == h1 + 3:
            wait(self.rs3(par))
            mine = near(self.p3 * self.u3, self.u3)
            total = self.s2[par, mine, :]
            for off in range(1, self.n3):
                total = total + self.r3[par, off].astype(f32)
            whole = total.astype(bf)
            self.o3[par, mine, :] = whole
            if squares is not None:
                wide = whole.astype(f32)
                squares[self.number] = squares[self.number] + wide * wide
            start(self.ag3(par))
        elif e == h1 + 4:
            wait(self.ag3(par))
            self.o2[third, near(self.p2 * self.u2, self.u2), :] = self.o3[par, :self.u2, :]
            start(self.ag2(1, par, third))
        elif e == h1 + 5:
            wait(self.ag2(1, par, third))
            start(self.ag2(2, par, third))
        else:
            t = e - (h1 + 6)
            if t == 0:
                wait(self.ag2(2, par, third))
                self.o[os, near(self.p1 * self.u1, self.u1), :] = self.o2[third, :self.u1, :]
            elif t <= h1:
                wait(self.ag1(t, par, os))
            if t < h1:
                start(self.ag1(t + 1, par, os))
            elif t == h1:
                self.output(c, os).start()
            else:
                self.output(c, os).wait()


def barrier(me):
    sem = pltpu.get_barrier_semaphore()
    count = 0
    for d in "xyz":
        p = place(me, d)
        for off in range(1, SIZE[d]):
            other = me + (lax.rem(p + off, SIZE[d]) - p) * STRIDE[d]
            pl.semaphore_signal(sem, inc=1, device_id={"dp": other}, device_id_type=MESH)
            count += 1
    pl.semaphore_wait(sem, count)


LAST = MLP + HEADS + 1
SENT = (MLP + 1, MLP + 6, LAST + 1)
BLOCKS = MLP + 3
PER, SPACING = 4, 3
SQUARES = SENT[2] + 4
ROUNDS = SENT[2] + 9


def started(m):
    return jnp.minimum(m - 1, MLP) + m // SENT[1] + m // SENT[2], (m >= 1) & ((m <= SENT[0]) | (m == SENT[1]) | (m == SENT[2]))


def poll(colours, squares, i, j):
    for colour in colours:
        for e in range(colour.last + 2):
            if (SPACING * e - j) % PER == 0:
                block, there = started(i - (SPACING * e - j) // PER)
                if colour.number == 2:
                    there &= block < BLOCKS - 1

                @pl.when(there)
                def _():
                    colour.event(e, block, squares)


def exchange(j, mine, came, sems, me):
    def copies(dim):
        p, n = place(me, dim), SIZE[dim]
        for off in range(1, n):
            there = lax.rem(p + off, n)
            at = "zyx".index(dim)
            yield pltpu.make_async_remote_copy(mine, came.at[at, p], sems.at[0, at, off], sems.at[1, at, off],
                                               device_id={"dp": me + (there - p) * STRIDE[dim]}, device_id_type=MESH)

    if j > 0:
        dim = "zyx"[j - 1]
        for copy in copies(dim):
            copy.wait()
        came[j - 1, place(me, dim)] = mine[...]
        total = came[j - 1, 0]
        for n in range(1, SIZE[dim]):
            total = total + came[j - 1, n]
        mine[...] = total
    if j < 3:
        for copy in copies("zyx"[j]):
            copy.start()


def mlp_tile(t, x1, x3, wg, wu, wd, ff, dgu):
    at = [rows(n * TOKENS + t * TILE, TILE) for n in range(HEADS)]
    b = jnp.concatenate([x1[a, :] for a in at], 1)
    dy = jnp.concatenate([x3[a, :] for a in at], 1)
    gate, upper = dot(b, wg[...]), dot(b, wu[...])
    by_f = dot_t(dy, wd[...]).astype(BF).astype(F32)
    gain = 1 / (1 + jnp.exp(-gate))
    act = gate * gain
    here = rows(t * TILE, TILE)
    ff[here, :] = (act * upper).astype(BF)
    dgu[here, :STEP] = (by_f * upper * (gain * (1 + gate * (1 - gain)))).astype(BF)
    dgu[here, STEP:] = (by_f * act).astype(BF)


def add_input_gradient(t, wg, wu, dgu, db):
    here = rows(t * TILE * 2, TILE * 2)
    part = dot_t(dgu[here, :], jnp.concatenate([wg[...], wu[...]], 1))
    for n, column in enumerate(columns(part)):
        at = rows(n * TOKENS + t * TILE * 2, TILE * 2)
        db[at, :] = db[at, :] + column


def turned_block(ref):
    return jnp.concatenate([ref[n * D : (n + 1) * D, :] for n in range(CHUNKS)], 1)


def put(g, slot, colour, half, w):
    for n, column in enumerate(columns(w)):
        g[slot, colour, (half + n) * D : (half + n + 1) * D, :] = column.astype(BF)


def residual_tile(t, x1, x3, x4, db, h, wo, delta):
    at = [rows(n * TOKENS + t * TILE, TILE) for n in range(HEADS)]
    by_b = jnp.concatenate([db[a, :] for a in at], 1).astype(BF).astype(F32)
    wide = h[t % 2].astype(F32)
    _, scale = normed(h[t % 2])
    by_h = (scale * by_b - wide * (scale * scale * scale * jnp.mean(by_b * wide, -1, keepdims=True))).astype(BF)
    by_h = (by_h.astype(F32) + jnp.concatenate([x3[a, :] for a in at], 1).astype(F32)).astype(BF)
    for a, column in zip(at, columns(by_h)):
        x3[a, :] = column
    by_att = dot_t(by_h, wo[...]).astype(BF)
    for n, column in enumerate(columns(by_att)):
        delta[n : n + 1, t * TILE : (t + 1) * TILE] = jnp.sum((column.astype(F32) * x1[at[n], :].astype(F32)).T, 0, keepdims=True)
        x4[at[n], :] = column


WIDE, STRIP = 1024, 256


def attention_block(head, first, key, many, strips, edge, x1, x4, k, v, db, dq, lse, delta):
    kk, vv = k[rows(key, many), :], v[rows(key, many), :]
    at = [rows(head * TOKENS + first + s, STRIP) for s in strips]
    qs, dos = [x1[a, :] for a in at], [x4[a, :] for a in at]
    scores, dps = [dot_t(kk, q) for q in qs], [dot_t(vv, d) for d in dos]
    dk = dv = None
    for n, s in enumerate(strips):
        here = pl.ds(first + s, STRIP)
        p = jnp.exp2(scores[n] * E - lse[pl.ds(head, 1), here] * (E / SCALE))
        if edge and n == 0:
            shape = (STRIP, STRIP)
            p = jnp.where(lax.broadcasted_iota(jnp.int32, shape, 1) >= lax.broadcasted_iota(jnp.int32, shape, 0), p, 0.0)
        ds = (p * (dps[n] - delta[pl.ds(head, 1), here])).astype(BF)
        a, b = dot(p.astype(BF), dos[n]), dot(ds, qs[n])
        dv, dk = (a, b) if dv is None else (dv + a, dk + b)
        dq[:, s : s + STRIP] += dot(kk.T, ds)
    for base, part in ((0, dk), (TOKENS, dv)):
        db[pl.ds(pl.multiple_of(base + key, STRIP), many), :] += part


def turn_back(t, first, cos, sin):
    here = pl.ds(first, t.shape[0])
    t = t.astype(BF).astype(F32)
    return (t * cos[here, :] - pltpu.roll(t, HALF, 1) * sin[here, :]).astype(BF)


def backward_kernel(b_hbm, bt_hbm, dy_hbm, dyt_hbm, h_hbm, att_hbm, attt_hbm, q_hbm, k_hbm, v_hbm, at_hbm, lse_hbm, cos_hbm, sin_hbm,
                    wg_hbm, wu_hbm, wd_hbm, wo_hbm, g_hbm, sq_hbm,
                    x1, x2, x3, x4, db, ff, dgu, wg, wu, wd, g, k, v, lse, delta, cos, sin, wo, h, dq, squares, total, came,
                    sem_x, sem_w, sem_in, sem_h, sem_sq, *rest):
    me = lax.axis_index("dp")
    barrier(me)
    colours, at = [Colour(dims) for dims in COLOURS], 0
    for number, colour in enumerate(colours):
        many = len(colour.scratch())
        colour.bind(rest[at : at + many], g, number, me, g_hbm)
        at += many

    def load(src, dst, sem):
        return pltpu.make_async_copy(src, dst, sem)

    first = [load(b_hbm, x1, sem_x.at[0]), load(bt_hbm, x2, sem_x.at[1]), load(dyt_hbm, x4, sem_x.at[2])]
    dys = [load(dy_hbm.at[0, :, pl.ds(n * LANE, LANE)], x3.at[pl.ds(n * TOKENS, TOKENS)], sem_x.at[3 + n]) for n in range(HEADS)]
    later = [load(src, dst, sem_in.at[n]) for n, (src, dst) in enumerate(((k_hbm, k), (v_hbm, v), (lse_hbm, lse), (cos_hbm, cos), (sin_hbm, sin), (wo_hbm.at[0], wo)))]
    swaps = [load(src, dst, sem_x.at[n]) for n, (src, dst) in enumerate(((att_hbm, x1), (attt_hbm, x2), (q_hbm, x1), (at_hbm, x2)))]

    def weights(i):
        par, cols = lax.rem(i, 2), rows(i * STEP, STEP)
        return [load(src, dst.at[par], sem_w.at[par, n]) for n, (src, dst) in enumerate(
            ((wg_hbm.at[0, :, cols], wg), (wu_hbm.at[0, :, cols], wu), (wd_hbm.at[0, cols, :], wd)))]

    def tile(t):
        return load(h_hbm.at[pl.ds(t * TILE, TILE)], h.at[t % 2], sem_h.at[t % 2])

    for copy in weights(0) + [first[0]] + dys + first[1:] + later:
        copy.start()
    db[...] = jnp.zeros_like(db)
    squares[...] = jnp.zeros_like(squares)
    for colour in colours:
        colour.zero()
    for copy in [first[0]] + dys:
        copy.wait()

    def body(i, _):
        par = lax.rem(i, 2)
        busy = (wg.at[par], wu.at[par], wd.at[par])

        def part(j):
            poll(colours, squares, i, j)

            @pl.when(i < MLP)
            def _():
                if j == 0:
                    for copy in weights(i):
                        copy.wait()

                    @pl.when(i + 1 < MLP)
                    def _():
                        for copy in weights(i + 1):
                            copy.start()

                if j < 2:
                    def two(t, _):
                        mlp_tile(t, x1, x3, *busy, ff, dgu)
                    lax.fori_loop(2 * j, 2 * j + 2, two, None)
                elif j == 2:
                    @pl.when(i == MLP - 1)
                    def _():
                        swaps[0].start()
                        for t in range(2):
                            tile(t).start()

                    def half(t, _):
                        add_input_gradient(t, busy[0], busy[1], dgu, db)
                    lax.fori_loop(0, 2, half, None)
                else:
                    @pl.when(i == 0)
                    def _():
                        for copy in first[1:]:
                            copy.wait()

                    slot = lax.rem(i, GS)
                    put(g, slot, 0, 0, dot(turned_block(x4), ff[...]))
                    put(g, slot, 1, 0, dot(turned_block(x2), dgu[:, :STEP]))
                    put(g, slot, 2, 0, dot(turned_block(x2), dgu[:, STEP:]))

            @pl.when(i == MLP)
            def _():
                if j == 0:
                    swaps[1].start()
                    swaps[0].wait()
                    for copy in later:
                        copy.wait()
                if j < 2:
                    for t in (2 * j, 2 * j + 1):
                        tile(t).wait()
                        residual_tile(t, x1, x3, x4, db, h, wo, delta)
                        if j == 0:
                            tile(t + 2).start()
                elif j == 2:
                    swaps[2].start()
                    swaps[1].wait()
                    db[: 2 * TOKENS, :] = jnp.zeros((2 * TOKENS, LANE), F32)
                if j >= 2:
                    def by_wo(n):
                        return dot(turned_block(x2), jnp.concatenate([x3[m * TOKENS : (m + 1) * TOKENS, :] for m in range(n, min(n + 2, HEADS))], 1))
                    for n in ((0, 2), (4, 6))[j - 2]:
                        put(g, (MLP + n // 6) % GS, (n // 2) % 3, 0, by_wo(n))
                if j == 3:
                    swaps[3].start()
                    swaps[2].wait()

            head = i - MLP - 1

            @pl.when((head >= 0) & (head < HEADS))
            def _():
                refs = (x1, x4, k, v, db, dq, lse, delta)
                late = WIDE if j in (1, 2) else 0
                if j < 2:
                    dq[...] = jnp.zeros_like(dq)
                if j == 1:
                    def seen(n, _):
                        attention_block(head, WIDE, n * TILE, TILE, range(0, WIDE, STRIP), False, *refs)
                    lax.fori_loop(0, 2, seen, None)
                if j in (0, 2):
                    for key in range(0, WIDE, STRIP):
                        attention_block(head, late, late + key, STRIP, range(key, WIDE, STRIP), True, *refs)
                    x3[rows(head * TOKENS + late, WIDE), :] = turn_back((dq[...] * SCALE).T, late, cos, sin)
                if j == 3:
                    @pl.when(head == 0)
                    def _():
                        swaps[3].wait()

                    def by_wq(n, many):
                        return dot(turned_block(x2), jnp.concatenate([x3[m * TOKENS : (m + 1) * TOKENS, :] for m in range(n, n + many)], 1))

                    for n in range(0, HEADS, 2):
                        @pl.when(head == n)
                        def _():
                            block = MLP + 1 + n // 6
                            if n == 0:
                                put(g, block % GS, 0, 1, by_wq(0, 1))
                            else:
                                put(g, block % GS, (n // 2) % 3, 0, by_wq(n - 1, 2))

            @pl.when(i == LAST)
            def _():
                if j < 2:
                    part = db[j * TOKENS : (j + 1) * TOKENS, :]
                    x1[j * TOKENS : (j + 1) * TOKENS, :] = part.astype(BF) if j else turn_back(part * SCALE, 0, cos, sin)
                elif j == 2:
                    both = jnp.concatenate([x1[:TOKENS, :], x1[TOKENS : 2 * TOKENS, :]], 1)
                    put(g, (BLOCKS - 1) % GS, 1, 0, dot(turned_block(x2), both))

            if j == 0:
                for step in range(4):
                    @pl.when(i == SQUARES + step)
                    def _():
                        if step == 0:
                            wide = squares[0] + squares[1] + squares[2]
                            total[...] = wide[:8, :] + wide[8:, :]
                        exchange(step, total, came, sem_sq, me)

        for j in range(PER):
            part(j)
        return None

    lax.fori_loop(0, ROUNDS, body, None)
    copy = load(total, sq_hbm, sem_in.at[0])
    copy.start()
    copy.wait()


def backward(args):
    flat = pltpu.VMEM((FLAT, LANE), BF)
    narrow = pltpu.VMEM((TOKENS, LANE), BF)
    table, heads = pltpu.VMEM((TOKENS, LANE), F32), pltpu.VMEM((HEADS, TOKENS), F32)
    sem = pltpu.SemaphoreType.DMA
    return pl.pallas_call(
        backward_kernel,
        in_specs=[ANY] * len(args),
        out_specs=[ANY] * 2,
        out_shape=[like(BLOCKS, len(COLOURS), ROWS, LANE), like(8, LANE, dtype=F32)],
        scratch_shapes=[flat] * 4
        + [pltpu.VMEM((FLAT, LANE), F32), pltpu.VMEM((TOKENS, STEP), BF), pltpu.VMEM((TOKENS, 2 * STEP), BF)]
        + [pltpu.VMEM((2, D, STEP), BF)] * 2
        + [pltpu.VMEM((2, STEP, D), BF), pltpu.VMEM((GS, len(COLOURS), ROWS, LANE), BF), narrow, narrow, heads, heads, table, table]
        + [pltpu.VMEM((D, D), BF), pltpu.VMEM((2, TILE, D), BF), pltpu.VMEM((LANE, WIDE), F32), pltpu.VMEM((3, 16, LANE), F32)]
        + [pltpu.VMEM((8, LANE), F32), pltpu.VMEM((3, 8, 8, LANE), F32), sem((10,)), sem((2, 3)), sem((6,)), sem((2,)), sem((2, 3, 8))]
        + [s for dims in COLOURS for s in Colour(dims).scratch()],
        compiler_params=pltpu.CompilerParams(collective_id=0, has_side_effects=True, vmem_limit_bytes=63 * MIB),
        cost_estimate=cost(16 * TOKENS * D * FF, 120),
    )(*args)


def clip(sq_ref, count):
    total = jnp.sum(jnp.sum(sq_ref[...], 0, keepdims=True), 1, keepdims=True)
    return jnp.minimum(1.0, 0.5 * lax.rsqrt(total / count + 1e-30))


def adamw(w, m, v, new_w, new_m, new_v, g):
    m = 0.9 * m[0] + 0.1 * g
    v = 0.95 * v[0] + 0.05 * g * g
    wide = w[0].astype(F32)
    new_w[0] = (wide - 0.02 * (m * lax.rsqrt(v + 1e-8) + 0.1 * wide)).astype(BF)
    new_m[0], new_v[0] = m, v


def update_mlp_kernel(count, sq_ref, g_ref, *refs):
    factor = clip(sq_ref, count)
    down, gate, upper = ([g_ref[0, n, k : k + D, :].astype(F32) * factor for k in (0, D)] for n in range(3))
    for n, g in enumerate((jnp.concatenate([part.T for part in down]), jnp.concatenate(gate, 1), jnp.concatenate(upper, 1))):
        adamw(*refs[n::3], g)


def update_rest_kernel(count, sq_ref, go_ref, gq_ref, gk_ref, gv_ref, *refs):
    factor = clip(sq_ref, count)
    for n, ref in enumerate((go_ref, gq_ref, gk_ref, gv_ref)):
        def one():
            adamw(*refs[n::4], ref[0].astype(F32) * factor)
        if n < 2:
            one()
        else:
            pl.when(pl.program_id(0) == 0)(one)


def update(kernel, steps, gs, specs, blocks, count, sq, arrays):
    return pl.pallas_call(
        functools.partial(kernel, count),
        grid=(steps,),
        in_specs=[whole((8, LANE))] + specs + blocks * 3,
        out_specs=blocks * 3,
        out_shape=[like(*a.shape, dtype=a.dtype) for a in arrays],
        compiler_params=pltpu.CompilerParams(vmem_limit_bytes=56 * MIB),
    )(sq, *gs, *arrays)


NAMES = ("wq", "wk", "wv", "wo", "w_gate", "w_up", "w_down")
IN_MLP, IN_ATTENTION = ("w_down", "w_gate", "w_up"), ("wo", "wq", "wk", "wv")


def block_of(shape, at):
    return pl.BlockSpec((1, *shape), at)


def along(i):
    return 0, 0, i


def gradient(first, step=1):
    return block_of((D, LANE), lambda i: (6 * MLP + first + step * i, 0, 0))


def solution(mesh):
    def step(x, dy, *arrays):
        kinds = [dict(zip(NAMES, arrays[n : n + len(NAMES)])) for n in range(0, len(arrays), len(NAMES))]
        w = kinds[0]
        cos, sin = tables()
        q, k, v, at = project(x, w["wq"], w["wk"], w["wv"], cos, sin)
        att, lse = attend(q, k, v)
        h, b, bt, dyt, attt = middle(att, x, dy, w["wo"])
        flat = lambda a: a.reshape(FLAT, LANE)
        g, sq = backward((flat(b), flat(bt), dy, flat(dyt), h, flat(att), flat(attt), flat(q), k, v, flat(at), lse, cos, sin,
                          w["w_gate"], w["w_up"], w["w_down"], w["wo"]))
        count = sum(a.size for a in w.values())
        wide, tall = block_of((D, STEP), along), block_of((STEP, D), lambda i: (0, i, 0))
        narrow, fixed = block_of((D, LANE), along), whole((1, D, LANE))
        new = {}
        for names, *rest in ((IN_MLP, update_mlp_kernel, MLP, [g], [block_of(g.shape[1:], lambda i: (i, 0, 0, 0))], [tall, wide, wide]),
                             (IN_ATTENTION, update_rest_kernel, HEADS, [g.reshape(-1, D, LANE)] * 4,
                              [gradient(0), gradient(HEADS), gradient(2 * HEADS, 0), gradient(2 * HEADS + 1, 0)], [narrow, narrow, fixed, fixed])):
            done = update(*rest, count, sq, [kind[name] for kind in kinds for name in names])
            new.update(zip([(n, name) for n in range(len(kinds)) for name in names], done))
        return tuple(new[n, name] for n in range(len(kinds)) for name in NAMES)

    states, all_of, ours = P(("rep", "dp"), None, None), P(None, None, None), P("rep", None, None)
    many = 3 * len(NAMES)
    return jax.shard_map(step, mesh=mesh, in_specs=(states, states) + (all_of,) * many, out_specs=(ours,) * many, check_vma=False)
```

```python
import functools

import jax
import jax.numpy as jnp
import numpy as np
from jax import lax
from jax.experimental import pallas as pl
from jax.experimental.pallas import tpu as pltpu
from jax.sharding import PartitionSpec as P

BF, F32 = jnp.bfloat16, jnp.float32
MESH = pl.DeviceIdType.MESH
ANY = pl.BlockSpec(memory_space=pl.ANY)
LANE, HALF = 128, 64
D, HEADS, FF, TOKENS = 896, 7, 2560, 2048
THETA = 10000
TILE = 512
WIDE, STRIP = 1024, 256
CHUNKS = TOKENS // LANE
FLAT = HEADS * TOKENS
STEP = 256
MLP = FF // STEP
TINY = 1e-6
SCALE = LANE**-0.5
E = SCALE * 1.4426950408889634
NEG = -1e30
MIB = 2**20


def dot(a, b, ca=1, cb=0):
    return lax.dot_general(a, b, (((ca,), (cb,)), ((), ())), preferred_element_type=F32)


def normed(h):
    wide = h.astype(F32)
    scale = lax.rsqrt(jnp.mean(wide * wide, -1, keepdims=True) + TINY)
    return (wide * scale).astype(BF), scale


def dot_t(a, b):
    return dot(a, b, 1, 1)


def columns(a):
    return [a[:, n : n + LANE] for n in range(0, a.shape[1], LANE)]


def rows(start, size):
    return pl.ds(start if isinstance(start, int) else pl.multiple_of(start, size), size)


def tables():
    angle = np.arange(TOKENS, dtype=np.float64)[:, None] * THETA ** (-np.arange(HALF, dtype=np.float64) / HALF)
    cos, sin = np.cos(angle), np.sin(angle)
    return jnp.asarray(np.concatenate([cos, cos], 1), F32), jnp.asarray(np.concatenate([-sin, sin], 1), F32)


def project_kernel(x_ref, cos_ref, sin_ref, wq_ref, wk_ref, wv_ref, q_ref, k_ref, v_ref, at_ref):
    a, _ = normed(x_ref[0])
    for n, part in enumerate(columns(a.T)):
        at_ref[n] = part

    def turned(t):
        t = t.astype(BF).astype(F32)
        return (t * cos_ref[...] + pltpu.roll(t, HALF, 1) * sin_ref[...]).astype(BF)

    for n, part in enumerate(columns(dot(a, wq_ref[0]))):
        q_ref[n] = turned(part)
    k_ref[...] = turned(dot(a, wk_ref[0]))
    v_ref[...] = dot(a, wv_ref[0]).astype(BF)


def cost(flops, megabytes):
    return pl.CostEstimate(flops=flops, bytes_accessed=megabytes * MIB, transcendentals=0)


def like(*shape, dtype=BF):
    return jax.ShapeDtypeStruct(shape, dtype)


def whole(shape):
    return pl.BlockSpec(shape, lambda i: (0,) * len(shape))


TILES = pl.BlockSpec((1, TILE, D), lambda i: (0, i, 0))
NARROW = pl.BlockSpec((TILE, LANE), lambda i: (i, 0))
SPLIT = pl.BlockSpec((HEADS, TILE, LANE), lambda i: (0, i, 0))
TURNED = pl.BlockSpec((TILE // LANE, D, LANE), lambda i: (i, 0, 0))
ROOM = pltpu.CompilerParams(vmem_limit_bytes=63 * MIB)
STEPS = (TOKENS // TILE,)


def project(x, wq, wk, wv, cos, sin):
    return pl.pallas_call(
        project_kernel,
        grid=STEPS,
        in_specs=[TILES, NARROW, NARROW, whole((1, D, D)), whole((1, D, LANE)), whole((1, D, LANE))],
        out_specs=[SPLIT, NARROW, NARROW, TURNED],
        out_shape=[like(HEADS, TOKENS, LANE), like(TOKENS, LANE), like(TOKENS, LANE), like(CHUNKS, D, LANE)],
        compiler_params=ROOM,
        cost_estimate=cost(2 * TOKENS * D * (D + 2 * LANE), 12),
    )(x, cos, sin, wq, wk, wv)


def attend_kernel(q_ref, k_ref, v_ref, o_ref, ot_ref, lse_ref, top_s, mix_s):
    iq = pl.program_id(0)
    top_s[...] = jnp.full_like(top_s, NEG)
    mix_s[...] = jnp.zeros_like(mix_s)
    ones = jnp.ones((8, TILE), BF)

    def block(j, masked):
        here = rows(j * TILE, TILE)
        scores = [dot_t(k_ref[here, :], q_ref[n]) for n in range(HEADS)]
        if masked:
            gap = lax.broadcasted_iota(jnp.int32, (TILE, TILE), 1) - lax.broadcasted_iota(jnp.int32, (TILE, TILE), 0)
        weights, keeps = [], []
        for n, s in enumerate(scores):
            if masked:
                s = jnp.where(gap >= 0, s, 2 * NEG)
            old = top_s[n : n + 1, :]
            top = jnp.maximum(old, s.max(axis=0, keepdims=True))
            top_s[n : n + 1, :] = top
            weights.append(jnp.exp2((s - top) * E).astype(BF))
            keeps.append(jnp.exp2((old - top) * E))
        values = jnp.concatenate([v_ref[here, :].T, ones], axis=0)
        for n in range(HEADS):
            mix_s[n] = mix_s[n] * keeps[n] + dot(values, weights[n])

    lax.fori_loop(0, iq, lambda j, _: block(j, False), None)
    block(iq, True)
    for n in range(HEADS):
        total = mix_s[n, LANE : LANE + 1, :]
        out = (mix_s[n, :LANE, :] * (1 / total)).astype(BF)
        o_ref[n] = out.T
        for m, part in enumerate(columns(out)):
            ot_ref[m, n * LANE : (n + 1) * LANE, :] = part
        lse_ref[n : n + 1, :] = top_s[n : n + 1, :] * SCALE + jnp.log(total)


def attend(q, k, v):
    return pl.pallas_call(
        attend_kernel,
        grid=STEPS,
        in_specs=[SPLIT, whole((TOKENS, LANE)), whole((TOKENS, LANE))],
        out_specs=[SPLIT, TURNED, pl.BlockSpec((HEADS, TILE), lambda i: (0, i))],
        out_shape=[like(HEADS, TOKENS, LANE), like(CHUNKS, D, LANE), like(HEADS, TOKENS, dtype=F32)],
        scratch_shapes=[pltpu.VMEM((HEADS, TILE), F32), pltpu.VMEM((HEADS, LANE + 8, TILE), F32)],
        compiler_params=ROOM,
        cost_estimate=cost(4 * HEADS * TOKENS * TOKENS * LANE, 8),
    )(q, k, v)


ROWS = 1792
SIZE = {"x": 4, "y": 4, "z": 8}
STRIDE = {"x": 32, "y": 8, "z": 1}
COLOURS = ("xyz", "yxz", "zxy")
GS = 4


def up(n, m):
    return -(-n // m) * m


FIRST, SECOND, THIRD = range(3)
WAYS = 0, 1
UP, DOWN = WAYS


def place(me, dim):
    return (me // STRIDE[dim]) % SIZE[dim]


def turn(way):
    return 1 - 2 * way


def near(first, size):
    return pl.ds(pl.multiple_of(first, LANE if size == LANE else 16), size)


def start(copies):
    for copy in copies:
        copy.start()


def wait(copies):
    for copy in copies:
        copy.wait()


class Colour:
    def __init__(self, dims):
        self.dims = dims
        self.n = self.n1, self.n2, self.n3 = [SIZE[d] for d in dims]
        self.u1 = ROWS // self.n1
        self.pad1 = up(self.u1, self.n2 * 16)
        self.u2 = self.pad1 // self.n2
        self.pad2 = up(self.u2, self.n3 * 16)
        self.u3 = self.pad2 // self.n3
        self.h1, self.h2 = self.n1 // 2, self.n2 // 2
        self.half1 = up(self.u1 // 2, 16)
        self.half2 = up(self.u2 // 2, 16)
        self.slots = 3 + self.h1 // 2
        self.last = 2 * self.h1 + 6

    def scratch(self):
        def twice(*shape, dtype=BF):
            return pltpu.VMEM((2, *shape, LANE), dtype)

        def sems(*shape):
            return pltpu.SemaphoreType.DMA((2, 2, *shape))

        r1, r2 = self.half1 + (self.h1 - 1) * self.u1, self.half2 + (self.h2 - 1) * self.u2
        ways = len(WAYS)
        return [
            twice(ways, r1),
            twice(self.pad1, dtype=F32),
            twice(ways + 1, self.u2),
            twice(ways, r2),
            twice(self.pad2, dtype=F32),
            twice(self.pad2),
            twice(self.n3, self.u3),
            twice(self.pad2),
            pltpu.VMEM((3, self.pad1, LANE), BF),
            pltpu.VMEM((self.slots, ROWS, LANE), BF),
            sems(ways, self.h1),
            sems(ways, self.h2),
            sems(self.n3),
            sems(self.n3),
            sems(ways, self.h2),
            sems(ways, self.h1),
            sems(),
        ]

    def bind(self, refs, g_ref, number, me, out):
        (self.r1, self.s1, self.t2, self.r2, self.s2, self.t3, self.r3, self.o3, self.o2, self.o,
         self.q1, self.q2, self.q3, self.a3, self.a2, self.a1, self.qo) = refs
        self.g, self.number, self.out, self.me = g_ref, number, out, me
        self.p = self.p1, self.p2, self.p3 = [place(me, d) for d in self.dims]

    def peer(self, k, off):
        d, n = self.dims[k], self.n[k]
        return {"dp": self.me + (lax.rem(self.p[k] + off + n, n) - self.p[k]) * STRIDE[d]}

    def zero(self):
        for ref in (self.s1, self.s2):
            ref[...] = jnp.zeros_like(ref)

    def _ring(self, k, src, dst, sems, par, way, step):
        return pltpu.make_async_remote_copy(src, dst, sems.at[0, par, way, step], sems.at[1, par, way, step],
                                            device_id=self.peer(k, turn(way)), device_id_type=MESH)

    def _span(self, halved, t, way, u, half):
        first, size = (0, u) if not halved else (0, half) if way == UP else (half, u - half)
        return first, size, max(half + (t - 2) * u, 0) if t > 1 else 0

    def rs1(self, t, way, gs, par):
        n, u = self.n1, self.u1
        dest = lax.rem(self.p1 + turn(way) * (self.h1 + 1 - t) + n, n)
        first, size, at = self._span(t == 1, t, way, u, self.half1)
        return self._ring(FIRST, self.g.at[gs, self.number, near(dest * u + first, size)], self.r1.at[par, way, pl.ds(at, size)], self.q1, par, way, t - 1)

    def rs2(self, t, way, par):
        first, size, at = self._span(t == 1, t, way, self.u2, self.half2)
        return self._ring(SECOND, self.t2.at[par, len(WAYS) if t == 1 else way, pl.ds(first, size)], self.r2.at[par, way, pl.ds(at, size)], self.q2, par, way, t - 1)

    def rs3(self, par):
        n, u = self.n3, self.u3
        return [pltpu.make_async_remote_copy(self.t3.at[par, near(lax.rem(self.p3 + off, n) * u, u)], self.r3.at[par, off], self.q3.at[0, par, off],
                                             self.q3.at[1, par, off], device_id=self.peer(THIRD, off), device_id_type=MESH) for off in range(1, n)]

    def ag3(self, par):
        mine = self.o3.at[par, near(self.p3 * self.u3, self.u3)]
        return [pltpu.make_async_remote_copy(mine, mine, self.a3.at[0, par, off], self.a3.at[1, par, off], device_id=self.peer(THIRD, off),
                                             device_id_type=MESH) for off in range(1, self.n3)]

    def _ag(self, k, t, way, par, ref, u, half, h, sems):
        n = self.n[k]
        piece = lax.rem(self.p[k] - turn(way) * (t - 1) + n, n)
        first, size, _ = self._span(t == h, t, way, u, half)
        here = ref.at[near(piece * u + first, size)]
        return self._ring(k, here, here, sems, par, way, t - 1)

    def ag2(self, t, par, third):
        return [self._ag(SECOND, t, way, par, self.o2.at[third], self.u2, self.half2, self.h2, self.a2) for way in WAYS]

    def ag1(self, t, par, os):
        return [self._ag(FIRST, t, way, par, self.o.at[os], self.u1, self.half1, self.h1, self.a1) for way in WAYS]

    def output(self, c, os, act):
        for half in range(2):
            def go(to):
                act([pltpu.make_async_copy(self.o.at[os, pl.ds(half * D, D)], to, self.qo.at[lax.rem(c, 2), half])])

            at = self.number * 2 + half

            @pl.when(c < MLP)
            def _():
                down, *across = self.out[:-1]
                go(across[self.number - 1].at[:, near(c * STEP + half * LANE, LANE)] if self.number else down.at[c, half])

            @pl.when(c >= MLP)
            def _():
                go(self.out[-1].at[:, near(((c - MLP) * 6 + at) * LANE, LANE)])

    def event(self, e, c, squares=None):
        par, third, gs, os = lax.rem(c, 2), lax.rem(c, 3), lax.rem(c, GS), lax.rem(c, self.slots)
        h1, f32, bf = self.h1, F32, BF
        if e <= h1:
            if e > 0:
                wait(self.rs1(e, way, gs, par) for way in WAYS)
            if e < h1:
                for way in WAYS:
                    if e > 0:
                        n, h, u, half = self.n1, self.h1, self.u1, self.half1
                        first, many, came = self._span(e == 1, e, way, u, half)
                        dest = lax.rem(self.p1 + turn(way) * (h - e) + n, n)
                        into = near(dest * u + first, many)
                        self.g[gs, self.number, into, :] = (self.g[gs, self.number, into, :].astype(f32) + self.r1[par, way, came:came + many, :].astype(f32)).astype(bf)
                    self.rs1(e + 1, way, gs, par).start()
                return
            u = self.u1
            _, _, at = self._span(False, h1, UP, u, self.half1)
            self.s1[par, :u, :] = (self.g[gs, self.number, near(self.p1 * u, u), :].astype(f32) + self.r1[par, 0, at:at + u, :].astype(f32)
                                   + self.r1[par, 1, at:at + u, :].astype(f32))
            opposite = lax.rem(self.p2 + 2, 4)
            self.t2[par, 2] = self.s1[par, near(opposite * self.u2, self.u2), :].astype(bf)
            start(self.rs2(1, way, par) for way in WAYS)
        elif e == h1 + 1:
            wait(self.rs2(1, way, par) for way in WAYS)
            for way in WAYS:
                dest = lax.rem(self.p2 + turn(way) + 4, 4)
                base, half = dest * self.u2, self.half2
                lo = self.s1[par, near(base, half), :]
                hi = self.s1[par, near(base + half, self.u2 - half), :]
                if way == UP:
                    lo = lo + self.r2[par, 0, :half, :].astype(f32)
                else:
                    hi = hi + self.r2[par, 1, :self.u2 - half, :].astype(f32)
                self.t2[par, way, :half, :] = lo.astype(bf)
                self.t2[par, way, half:, :] = hi.astype(bf)
                self.rs2(2, way, par).start()
        elif e == h1 + 2:
            wait(self.rs2(2, way, par) for way in WAYS)
            u, at = self.u2, self.half2
            self.s2[par, :u, :] = (self.s1[par, near(self.p2 * u, u), :] + self.r2[par, 0, at:at + u, :].astype(f32)
                                   + self.r2[par, 1, at:at + u, :].astype(f32))
            self.t3[par] = self.s2[par].astype(bf)
            start(self.rs3(par))
        elif e == h1 + 3:
            wait(self.rs3(par))
            mine = near(self.p3 * self.u3, self.u3)
            total = self.s2[par, mine, :]
            for off in range(1, self.n3):
                total = total + self.r3[par, off].astype(f32)
            whole = total.astype(bf)
            self.o3[par, mine, :] = whole
            if squares is not None:
                wide = whole.astype(f32)
                squares[self.number] = squares[self.number] + wide * wide
            start(self.ag3(par))
        elif e == h1 + 4:
            wait(self.ag3(par))
            self.o2[third, near(self.p2 * self.u2, self.u2), :] = self.o3[par, :self.u2, :]
            start(self.ag2(1, par, third))
        elif e == h1 + 5:
            wait(self.ag2(1, par, third))
            start(self.ag2(2, par, third))
        else:
            t = e - (h1 + 6)
            if t == 0:
                wait(self.ag2(2, par, third))
                self.o[os, near(self.p1 * self.u1, self.u1), :] = self.o2[third, :self.u1, :]
            elif t <= h1:
                wait(self.ag1(t, par, os))
            if t < h1:
                start(self.ag1(t + 1, par, os))
            elif t == h1:
                self.output(c, os, start)
            else:
                self.output(c, os, wait)


def barrier(me):
    sem = pltpu.get_barrier_semaphore()
    count = 0
    for d in "xyz":
        p = place(me, d)
        for off in range(1, SIZE[d]):
            other = me + (lax.rem(p + off, SIZE[d]) - p) * STRIDE[d]
            pl.semaphore_signal(sem, inc=1, device_id={"dp": other}, device_id_type=MESH)
            count += 1
    pl.semaphore_wait(sem, count)


LAST = MLP + HEADS + 1
SENT = (MLP + 1, MLP + 6, LAST + 1)
BLOCKS = MLP + 3
PER, SPACING = 4, 3
SQUARES = SENT[2] + 4
ROUNDS = SENT[2] + 9


def started(m):
    return jnp.minimum(m - 1, MLP) + m // SENT[1] + m // SENT[2], (m >= 1) & ((m <= SENT[0]) | (m == SENT[1]) | (m == SENT[2]))


def poll(colours, squares, i, j):
    for colour in colours:
        for e in range(colour.last + 2):
            if (SPACING * e - j) % PER == 0:
                block, there = started(i - (SPACING * e - j) // PER)
                if colour.number == 2:
                    there &= block < BLOCKS - 1

                @pl.when(there)
                def _():
                    colour.event(e, block, squares)


def exchange(j, mine, came, sems, me):
    def copies(dim):
        p, n = place(me, dim), SIZE[dim]
        for off in range(1, n):
            there = lax.rem(p + off, n)
            at = "zyx".index(dim)
            yield pltpu.make_async_remote_copy(mine, came.at[at, p], sems.at[0, at, off], sems.at[1, at, off],
                                               device_id={"dp": me + (there - p) * STRIDE[dim]}, device_id_type=MESH)

    if j > 0:
        dim = "zyx"[j - 1]
        for copy in copies(dim):
            copy.wait()
        came[j - 1, place(me, dim)] = mine[...]
        total = came[j - 1, 0]
        for n in range(1, SIZE[dim]):
            total = total + came[j - 1, n]
        mine[...] = total
    if j < 3:
        for copy in copies("zyx"[j]):
            copy.start()


def stage(dgu, t, n):
    k = t % 2 * HEADS + n
    return dgu.at[pl.ds(k % 4 * TILE, TILE), pl.ds(k // 4 * LANE, LANE)]


def middle_tile(t, slot, x1, x2, x3, x4, dgu, xs, hs, wo):
    att = jnp.concatenate([stage(dgu, slot, n)[...] for n in range(HEADS)], 1)
    h = (xs[slot].astype(F32) + dot(att, wo[...]).astype(BF).astype(F32)).astype(BF)
    hs[rows(t * TILE, TILE), :] = h
    b, _ = normed(h)
    at = [rows(n * TOKENS + t * TILE, TILE) for n in range(HEADS)]
    for a, part in zip(at, columns(b)):
        x1[a, :] = part
    dy = jnp.concatenate([x3[a, :] for a in at], 1)
    for ref, a in ((x2, b), (x4, dy)):
        for n, part in enumerate(columns(a.T)):
            ref[pl.ds(pl.multiple_of(t * (TILE // LANE * D) + n * D, LANE), D), :] = part


def mlp_tile(t, x1, x3, wg, wu, wd, ff, dgu):
    at = [pl.ds(n * TOKENS + t * WIDE, WIDE) for n in range(HEADS)]
    b = jnp.concatenate([x1[a, :] for a in at], 1)
    dy = jnp.concatenate([x3[a, :] for a in at], 1)
    gate, upper = dot(b, wg[...]), dot(b, wu[...])
    by_f = dot_t(dy, wd[...]).astype(BF).astype(F32)
    gain = 1 / (1 + jnp.exp(-gate))
    act = gate * gain
    here = pl.ds(t * WIDE, WIDE)
    ff[here, :] = (act * upper).astype(BF)
    dgu[here, :STEP] = (by_f * upper * (gain * (1 + gate * (1 - gain)))).astype(BF)
    dgu[here, STEP:] = (by_f * act).astype(BF)


def add_input_gradient(t, wg, wu, dgu, db):
    here = rows(t * WIDE, WIDE)
    part = dot_t(dgu[here, :], jnp.concatenate([wg[...], wu[...]], 1))
    for n, column in enumerate(columns(part)):
        at = rows(n * TOKENS + t * WIDE, WIDE)
        db[at, :] = db[at, :] + column


def turned_block(ref):
    return jnp.concatenate([ref[n * D : (n + 1) * D, :] for n in range(CHUNKS)], 1)


def put(g, slot, colour, half, w):
    for n, column in enumerate(columns(w)):
        g[slot, colour, (half + n) * D : (half + n + 1) * D, :] = column.astype(BF)


def residual_tile(t, x1, x3, x4, db, hs, wo, delta):
    at = [rows(n * TOKENS + t * TILE, TILE) for n in range(HEADS)]
    by_b = jnp.concatenate([db[a, :] for a in at], 1).astype(BF).astype(F32)
    h = hs[t * TILE : (t + 1) * TILE, :]
    wide = h.astype(F32)
    _, scale = normed(h)
    by_h = (scale * by_b - wide * (scale * scale * scale * jnp.mean(by_b * wide, -1, keepdims=True))).astype(BF)
    by_h = (by_h.astype(F32) + jnp.concatenate([x3[a, :] for a in at], 1).astype(F32)).astype(BF)
    for a, column in zip(at, columns(by_h)):
        x3[a, :] = column
    by_att = dot_t(by_h, wo[...]).astype(BF)
    for n, column in enumerate(columns(by_att)):
        delta[n : n + 1, t * TILE : (t + 1) * TILE] = jnp.sum((column.astype(F32) * x1[at[n], :].astype(F32)).T, 0, keepdims=True)
        x4[at[n], :] = column


def attention_block(head, first, key, many, strips, edge, x1, x4, k, v, db, dq, lse, delta):
    kk, vv = k[rows(key, many), :], v[rows(key, many), :]
    at = [rows(head * TOKENS + first + s, STRIP) for s in strips]
    qs, dos = [x1[a, :] for a in at], [x4[a, :] for a in at]
    scores, dps = [dot_t(kk, q) for q in qs], [dot_t(vv, d) for d in dos]
    dk = dv = None
    for n, s in enumerate(strips):
        here = pl.ds(first + s, STRIP)
        p = jnp.exp2(scores[n] * E - lse[pl.ds(head, 1), here] * (E / SCALE))
        if edge and n == 0:
            shape = (STRIP, STRIP)
            p = jnp.where(lax.broadcasted_iota(jnp.int32, shape, 1) >= lax.broadcasted_iota(jnp.int32, shape, 0), p, 0.0)
        ds = (p * (dps[n] - delta[pl.ds(head, 1), here])).astype(BF)
        a, b = dot(p.astype(BF), dos[n]), dot(ds, qs[n])
        dv, dk = (a, b) if dv is None else (dv + a, dk + b)
        dq[:, s : s + STRIP] += dot(kk.T, ds)
    for base, part in ((0, dk), (TOKENS, dv)):
        db[pl.ds(pl.multiple_of(base + key, STRIP), many), :] += part


def turn_back(t, first, cos, sin):
    here = pl.ds(first, t.shape[0])
    t = t.astype(BF).astype(F32)
    return (t * cos[here, :] - pltpu.roll(t, HALF, 1) * sin[here, :]).astype(BF)


def backward_kernel(x_hbm, dy_hbm, att_hbm, attt_hbm, q_hbm, k_hbm, v_hbm, at_hbm, lse_hbm, cos_hbm, sin_hbm, wg_hbm, wu_hbm, wd_hbm, wo_hbm,
                    gd_hbm, gg_hbm, gu_hbm, ga_hbm, sq_hbm,
                    x1, x2, x3, x4, db, ff, dgu, wg, wu, wd, g, k, v, lse, delta, cos, sin, wo, xs, hs, dq, squares, total, came,
                    sem_x, sem_w, sem_in, sem_t, sem_sq, *rest):
    me = lax.axis_index("dp")
    barrier(me)
    colours, at = [Colour(dims) for dims in COLOURS], 0
    for number, colour in enumerate(colours):
        many = len(colour.scratch())
        colour.bind(rest[at : at + many], g, number, me, (gd_hbm, gg_hbm, gu_hbm, ga_hbm))
        at += many

    def load(src, dst, sem):
        return pltpu.make_async_copy(src, dst, sem)

    dys = [load(dy_hbm.at[0, :, pl.ds(n * LANE, LANE)], x3.at[pl.ds(n * TOKENS, TOKENS)], sem_x.at[n]) for n in range(HEADS)]
    first = load(wo_hbm.at[0], wo, sem_x.at[HEADS])
    later = [load(src, dst, sem_in.at[n]) for n, (src, dst) in enumerate(((k_hbm, k), (v_hbm, v), (lse_hbm, lse), (cos_hbm, cos), (sin_hbm, sin)))]
    swaps = [load(src, dst, sem_x.at[n]) for n, (src, dst) in enumerate(((att_hbm, x1), (attt_hbm, x2), (q_hbm, x1), (at_hbm, x2)))]

    def weights(i):
        par, cols = lax.rem(i, 2), rows(i * STEP, STEP)
        return [load(src, dst.at[par], sem_w.at[par, n]) for n, (src, dst) in enumerate(
            ((wg_hbm.at[0, :, cols], wg), (wu_hbm.at[0, :, cols], wu), (wd_hbm.at[0, cols, :], wd)))]

    def tile(t, slot):
        here = rows(t * TILE, TILE)
        heads = [load(att_hbm.at[pl.ds(n * TOKENS + pl.multiple_of(t * TILE, TILE), TILE)], stage(dgu, slot, n), sem_t.at[slot, n]) for n in range(HEADS)]
        return heads + [load(x_hbm.at[0, here], xs.at[slot], sem_t.at[slot, HEADS])]

    for copies in ([first], tile(0, 0), dys, tile(1, 1), weights(0), later):
        start(copies)
    db[...] = jnp.zeros_like(db)
    squares[...] = jnp.zeros_like(squares)
    for colour in colours:
        colour.zero()
    wait([first] + dys)

    def middle(n, _):
        for slot in range(2):
            t = 2 * n + slot
            wait(tile(t, slot))
            middle_tile(t, slot, x1, x2, x3, x4, dgu, xs, hs, wo)

            @pl.when(n == 0)
            def _():
                start(tile(t + 2, slot))

    lax.fori_loop(0, 2, middle, None)

    def body(i, _):
        par = lax.rem(i, 2)
        busy = (wg.at[par], wu.at[par], wd.at[par])

        def part(j):
            poll(colours, squares, i, j)

            @pl.when(i < MLP)
            def _():
                if j == 0:
                    wait(weights(i))

                    @pl.when(i + 1 < MLP)
                    def _():
                        start(weights(i + 1))

                if j < 2:
                    mlp_tile(j, x1, x3, *busy, ff, dgu)
                elif j == 2:
                    @pl.when(i == MLP - 1)
                    def _():
                        swaps[0].start()

                    def half(t, _):
                        add_input_gradient(t, busy[0], busy[1], dgu, db)
                    lax.fori_loop(0, 2, half, None)
                else:
                    slot = lax.rem(i, GS)
                    put(g, slot, 0, 0, dot(turned_block(x4), ff[...]))
                    put(g, slot, 1, 0, dot(turned_block(x2), dgu[:, :STEP]))
                    put(g, slot, 2, 0, dot(turned_block(x2), dgu[:, STEP:]))

            @pl.when(i == MLP)
            def _():
                if j == 0:
                    swaps[1].start()
                    swaps[0].wait()
                    wait(later)
                if j < 2:
                    for t in (2 * j, 2 * j + 1):
                        residual_tile(t, x1, x3, x4, db, hs, wo, delta)
                elif j == 2:
                    swaps[2].start()
                    swaps[1].wait()
                    db[: 2 * TOKENS, :] = jnp.zeros((2 * TOKENS, LANE), F32)
                if j >= 2:
                    def by_wo(n):
                        return dot(turned_block(x2), jnp.concatenate([x3[m * TOKENS : (m + 1) * TOKENS, :] for m in range(n, min(n + 2, HEADS))], 1))
                    for n in ((0, 2), (4, 6))[j - 2]:
                        put(g, (MLP + n // 6) % GS, (n // 2) % 3, 0, by_wo(n))
                if j == 3:
                    swaps[3].start()
                    swaps[2].wait()

            head = i - MLP - 1

            @pl.when((head >= 0) & (head < HEADS))
            def _():
                refs = (x1, x4, k, v, db, dq, lse, delta)
                late = WIDE if j in (1, 2) else 0
                if j < 2:
                    dq[...] = jnp.zeros_like(dq)
                if j == 1:
                    def seen(n, _):
                        attention_block(head, WIDE, n * TILE, TILE, range(0, WIDE, STRIP), False, *refs)
                    lax.fori_loop(0, 2, seen, None)
                if j in (0, 2):
                    for key in range(0, WIDE, STRIP):
                        attention_block(head, late, late + key, STRIP, range(key, WIDE, STRIP), True, *refs)
                    x3[rows(head * TOKENS + late, WIDE), :] = turn_back((dq[...] * SCALE).T, late, cos, sin)
                if j == 3:
                    @pl.when(head == 0)
                    def _():
                        swaps[3].wait()

                    def by_wq(n, many):
                        return dot(turned_block(x2), jnp.concatenate([x3[m * TOKENS : (m + 1) * TOKENS, :] for m in range(n, n + many)], 1))

                    for n in range(0, HEADS, 2):
                        @pl.when(head == n)
                        def _():
                            block = MLP + 1 + n // 6
                            if n == 0:
                                put(g, block % GS, 0, 1, by_wq(0, 1))
                            else:
                                put(g, block % GS, (n // 2) % 3, 0, by_wq(n - 1, 2))

            @pl.when(i == LAST)
            def _():
                if j < 2:
                    part = db[j * TOKENS : (j + 1) * TOKENS, :]
                    x1[j * TOKENS : (j + 1) * TOKENS, :] = part.astype(BF) if j else turn_back(part * SCALE, 0, cos, sin)
                elif j == 2:
                    both = jnp.concatenate([x1[:TOKENS, :], x1[TOKENS : 2 * TOKENS, :]], 1)
                    put(g, (BLOCKS - 1) % GS, 1, 0, dot(turned_block(x2), both))

            if j == 0:
                for step in range(4):
                    @pl.when(i == SQUARES + step)
                    def _():
                        if step == 0:
                            wide = squares[0] + squares[1] + squares[2]
                            total[...] = wide[:8, :] + wide[8:, :]
                        exchange(step, total, came, sem_sq, me)

        for j in range(PER):
            part(j)
        return None

    lax.fori_loop(0, ROUNDS, body, None)
    copy = load(total, sq_hbm, sem_in.at[0])
    copy.start()
    copy.wait()


def backward(args):
    flat = pltpu.VMEM((FLAT, LANE), BF)
    narrow = pltpu.VMEM((TOKENS, LANE), BF)
    table, heads = pltpu.VMEM((TOKENS, LANE), F32), pltpu.VMEM((HEADS, TOKENS), F32)
    sem = pltpu.SemaphoreType.DMA
    thirds = len(COLOURS)
    return pl.pallas_call(
        backward_kernel,
        in_specs=[ANY] * len(args),
        out_specs=[ANY] * 5,
        out_shape=[like(MLP, 2, D, LANE), like(D, FF), like(D, FF), like(D, 6 * thirds * LANE), like(8, LANE, dtype=F32)],
        scratch_shapes=[flat] * 4
        + [pltpu.VMEM((FLAT, LANE), F32), pltpu.VMEM((TOKENS, STEP), BF), pltpu.VMEM((TOKENS, 2 * STEP), BF)]
        + [pltpu.VMEM((2, D, STEP), BF)] * 2
        + [pltpu.VMEM((2, STEP, D), BF), pltpu.VMEM((GS, thirds, ROWS, LANE), BF), narrow, narrow, heads, heads, table, table]
        + [pltpu.VMEM((D, D), BF), pltpu.VMEM((2, TILE, D), BF), pltpu.VMEM((TOKENS, D), BF), pltpu.VMEM((LANE, WIDE), F32)]
        + [pltpu.VMEM((thirds, 16, LANE), F32), pltpu.VMEM((8, LANE), F32), pltpu.VMEM((thirds, 8, 8, LANE), F32)]
        + [sem((HEADS + 1,)), sem((2, thirds)), sem((5,)), sem((2, HEADS + 1)), sem((2, thirds, 8))]
        + [s for dims in COLOURS for s in Colour(dims).scratch()],
        compiler_params=pltpu.CompilerParams(collective_id=0, has_side_effects=True, vmem_limit_bytes=63 * MIB),
        cost_estimate=cost(16 * TOKENS * D * FF, 120),
    )(*args)


def adamw(w, m, v, new_w, new_m, new_v, g):
    m = 0.9 * m[0] + 0.1 * g
    v = 0.95 * v[0] + 0.05 * g * g
    wide = w[0].astype(F32)
    new_w[0] = (wide - 0.02 * (m * lax.rsqrt(v + 1e-8) + 0.1 * wide)).astype(BF)
    new_m[0], new_v[0] = m, v


ORDER = ("w_down", "w_gate", "w_up", "wo", "wq", "wk", "wv")
ROUNDS_OF_UPDATE = ((MLP, [(STEP, D)]), (14, [(D // 14, FF)] * 2), (HEADS, [(LANE, D)] * 2 + [(LANE, LANE)] * 2))


def update_kernel(count, sq_ref, *refs):
    total = jnp.sum(jnp.sum(sq_ref[...], 0, keepdims=True), 1, keepdims=True)
    factor = jnp.minimum(1.0, 0.5 * lax.rsqrt(total / count + 1e-30))
    names = len(ORDER)
    gs, refs = refs[:names], refs[names:]
    step, begin, n = pl.program_id(0), 0, 0
    for steps, blocks in ROUNDS_OF_UPDATE:
        @pl.when((step >= begin) & (step < begin + steps))
        def _():
            for k in range(n, n + len(blocks)):
                g = gs[k][...] if k else jnp.concatenate([gs[k][0, half].T for half in range(2)])
                adamw(*refs[k::names], g.astype(F32) * factor)
        begin, n = begin + steps, n + len(blocks)


def update(gs, sq, arrays, count):
    by_rows, gradients, begin = [], [], 0
    for steps, blocks in ROUNDS_OF_UPDATE:
        def turn_of(i, begin=begin, steps=steps):
            return jnp.clip(i - begin, 0, steps - 1)

        for shape in blocks:
            by_rows.append(pl.BlockSpec((1, *shape), lambda i, at=turn_of: (0, at(i), 0)))
            place = len(gradients) - 3
            if place < -2:
                gradients.append(pl.BlockSpec((1, 2, D, LANE), lambda i, at=turn_of: (at(i), 0, 0, 0)))
            else:
                gradients.append(pl.BlockSpec(shape, lambda i, at=turn_of, col=(0, 0, 0, 1, 2 * HEADS, 2 * HEADS + 1)[place + 2]: (at(i), col)))
        begin += steps
    return pl.pallas_call(
        functools.partial(update_kernel, count),
        grid=(begin,),
        in_specs=[whole((8, LANE))] + gradients + by_rows * 3,
        out_specs=by_rows * 3,
        out_shape=[like(*a.shape, dtype=a.dtype) for a in arrays],
        compiler_params=ROOM,
    )(sq, *gs[:3], *[gs[3]] * 4, *arrays)


NAMES = ("wq", "wk", "wv", "wo", "w_gate", "w_up", "w_down")


def solution(mesh):
    def step(x, dy, *arrays):
        kinds = [dict(zip(NAMES, arrays[n : n + len(NAMES)])) for n in range(0, len(arrays), len(NAMES))]
        w = kinds[0]
        cos, sin = tables()
        q, k, v, at = project(x, w["wq"], w["wk"], w["wv"], cos, sin)
        att, attt, lse = attend(q, k, v)
        flat = lambda a: a.reshape(FLAT, LANE)
        *gs, sq = backward((x, dy, flat(att), flat(attt), flat(q), k, v, flat(at), lse, cos, sin, w["w_gate"], w["w_up"], w["w_down"], w["wo"]))
        done = update(gs, sq, [kind[name] for kind in kinds for name in ORDER], sum(a.size for a in w.values()))
        new = dict(zip([(n, name) for n in range(len(kinds)) for name in ORDER], done))
        return tuple(new[n, name] for n in range(len(kinds)) for name in NAMES)

    states, all_of, ours = P(("rep", "dp"), None, None), P(None, None, None), P("rep", None, None)
    many = 3 * len(NAMES)
    return jax.shard_map(step, mesh=mesh, in_specs=(states, states) + (all_of,) * many, out_specs=(ours,) * many, check_vma=False)
```

```python
import functools

import jax
import jax.numpy as jnp
import numpy as np
from jax import lax
from jax.experimental import pallas as pl
from jax.experimental.pallas import tpu as pltpu
from jax.sharding import PartitionSpec as P

BF, F32 = jnp.bfloat16, jnp.float32
MESH = pl.DeviceIdType.MESH
ANY = pl.BlockSpec(memory_space=pl.ANY)
LANE, HALF = 128, 64
D, HEADS, FF, TOKENS = 896, 7, 2560, 2048
THETA = 10000
TILE = 512
WIDE, STRIP = 1024, 256
CHUNKS = TOKENS // LANE
FLAT = HEADS * TOKENS
STEP = 256
MLP = FF // STEP
TINY = 1e-6
SCALE = LANE**-0.5
E = SCALE * 1.4426950408889634
NEG = -1e30
MIB = 2**20


def dot(a, b, ca=1, cb=0):
    return lax.dot_general(a, b, (((ca,), (cb,)), ((), ())), preferred_element_type=F32)


def normed(h):
    wide = h.astype(F32)
    scale = lax.rsqrt(jnp.mean(wide * wide, -1, keepdims=True) + TINY)
    return (wide * scale).astype(BF), scale


def dot_t(a, b):
    return dot(a, b, 1, 1)


def columns(a):
    return [a[:, n : n + LANE] for n in range(0, a.shape[1], LANE)]


def rows(start, size):
    return pl.ds(start if isinstance(start, int) else pl.multiple_of(start, size), size)


def tables():
    angle = np.arange(TOKENS, dtype=np.float64)[:, None] * THETA ** (-np.arange(HALF, dtype=np.float64) / HALF)
    cos, sin = np.cos(angle), np.sin(angle)
    return jnp.asarray(np.concatenate([cos, cos], 1), F32), jnp.asarray(np.concatenate([-sin, sin], 1), F32)


def project_kernel(x_ref, cos_ref, sin_ref, wq_ref, wk_ref, wv_ref, q_ref, k_ref, v_ref, at_ref):
    a, _ = normed(x_ref[0])
    for n, part in enumerate(columns(a.T)):
        at_ref[n] = part

    def turned(t):
        t = t.astype(BF).astype(F32)
        return (t * cos_ref[...] + pltpu.roll(t, HALF, 1) * sin_ref[...]).astype(BF)

    for n, part in enumerate(columns(dot(a, wq_ref[0]))):
        q_ref[n] = turned(part)
    k_ref[...] = turned(dot(a, wk_ref[0]))
    v_ref[...] = dot(a, wv_ref[0]).astype(BF)


def cost(flops, megabytes):
    return pl.CostEstimate(flops=flops, bytes_accessed=megabytes * MIB, transcendentals=0)


def like(*shape, dtype=BF):
    return jax.ShapeDtypeStruct(shape, dtype)


def whole(shape):
    return pl.BlockSpec(shape, lambda i: (0,) * len(shape))


TILES = pl.BlockSpec((1, TILE, D), lambda i: (0, i, 0))
NARROW = pl.BlockSpec((TILE, LANE), lambda i: (i, 0))
SPLIT = pl.BlockSpec((HEADS, TILE, LANE), lambda i: (0, i, 0))
TURNED = pl.BlockSpec((TILE // LANE, D, LANE), lambda i: (i, 0, 0))
ROOM = pltpu.CompilerParams(vmem_limit_bytes=63 * MIB)
STEPS = (TOKENS // TILE,)


def project(x, wq, wk, wv, cos, sin):
    return pl.pallas_call(
        project_kernel,
        grid=STEPS,
        in_specs=[TILES, NARROW, NARROW, whole((1, D, D)), whole((1, D, LANE)), whole((1, D, LANE))],
        out_specs=[SPLIT, NARROW, NARROW, TURNED],
        out_shape=[like(HEADS, TOKENS, LANE), like(TOKENS, LANE), like(TOKENS, LANE), like(CHUNKS, D, LANE)],
        compiler_params=ROOM,
        cost_estimate=cost(2 * TOKENS * D * (D + 2 * LANE), 12),
    )(x, cos, sin, wq, wk, wv)


def attend_kernel(q_ref, k_ref, v_ref, o_ref, ot_ref, lse_ref, top_s, mix_s):
    iq = pl.program_id(0)
    top_s[...] = jnp.full_like(top_s, NEG)
    mix_s[...] = jnp.zeros_like(mix_s)

    def block(first, many, strips, edge):
        here, wide = pl.ds(first, many), TILE // 2 if edge else TILE
        pieces = [(n, s) for n in range(HEADS) for s in strips]
        keys = k_ref[here, :]
        scores = [dot_t(keys, q_ref[n, s : s + wide, :]) for n, s in pieces]
        weights, keeps = [], []
        for (n, s), score in zip(pieces, scores):
            if edge and s == strips[0]:
                shape = (many, wide)
                score = jnp.where(lax.broadcasted_iota(jnp.int32, shape, 1) >= lax.broadcasted_iota(jnp.int32, shape, 0), score, 2 * NEG)
            old = top_s[n : n + 1, s : s + wide]
            top = jnp.maximum(old, score.max(axis=0, keepdims=True))
            top_s[n : n + 1, s : s + wide] = top
            weights.append(jnp.exp2((score - top) * E).astype(BF))
            keeps.append(jnp.exp2((old - top) * E))
        values = jnp.concatenate([v_ref[here, :].T, jnp.ones((8, many), BF)], axis=0)
        for (n, s), p, keep in zip(pieces, weights, keeps):
            mix_s[n, :, s : s + wide] = mix_s[n, :, s : s + wide] * keep + dot(values, p)

    lax.fori_loop(0, iq, lambda j, _: block(pl.multiple_of(j * TILE, TILE), TILE, (0,), False), None)
    for s in (0, STRIP):
        block(pl.multiple_of(iq * TILE + s, STRIP), STRIP, range(s, TILE, STRIP), True)
    for n in range(HEADS):
        total = mix_s[n, LANE : LANE + 1, :]
        out = (mix_s[n, :LANE, :] * (1 / total)).astype(BF)
        o_ref[n] = out.T
        for m, part in enumerate(columns(out)):
            ot_ref[m, n * LANE : (n + 1) * LANE, :] = part
        lse_ref[n : n + 1, :] = top_s[n : n + 1, :] * SCALE + jnp.log(total)


def attend(q, k, v):
    return pl.pallas_call(
        attend_kernel,
        grid=STEPS,
        in_specs=[SPLIT, whole((TOKENS, LANE)), whole((TOKENS, LANE))],
        out_specs=[SPLIT, TURNED, pl.BlockSpec((HEADS, TILE), lambda i: (0, i))],
        out_shape=[like(HEADS, TOKENS, LANE), like(CHUNKS, D, LANE), like(HEADS, TOKENS, dtype=F32)],
        scratch_shapes=[pltpu.VMEM((HEADS, TILE), F32), pltpu.VMEM((HEADS, LANE + 8, TILE), F32)],
        compiler_params=ROOM,
        cost_estimate=cost(4 * HEADS * TOKENS * TOKENS * LANE, 8),
    )(q, k, v)


ROWS = 1792
SIZE = {"x": 4, "y": 4, "z": 8}
STRIDE = {"x": 32, "y": 8, "z": 1}
COLOURS = ("xyz", "yxz", "zxy")
GS = 4


def up(n, m):
    return -(-n // m) * m


FIRST, SECOND, THIRD = range(3)
WAYS = 0, 1
UP, DOWN = WAYS


def place(me, dim):
    return (me // STRIDE[dim]) % SIZE[dim]


def turn(way):
    return 1 - 2 * way


def near(first, size):
    return pl.ds(pl.multiple_of(first, LANE if size == LANE else 16), size)


def start(copies):
    for copy in copies:
        copy.start()


def wait(copies):
    for copy in copies:
        copy.wait()


class Colour:
    def __init__(self, dims):
        self.dims = dims
        self.n = self.n1, self.n2, self.n3 = [SIZE[d] for d in dims]
        self.u1 = ROWS // self.n1
        self.pad1 = up(self.u1, self.n2 * 16)
        self.u2 = self.pad1 // self.n2
        self.pad2 = up(self.u2, self.n3 * 16)
        self.u3 = self.pad2 // self.n3
        self.h1 = self.n1 // 2
        self.half1 = up(self.u1 // 2, 16)
        self.slots = 3 + self.h1 // 2
        self.last = 2 * self.h1 + 4

    def scratch(self):
        def twice(*shape, dtype=BF):
            return pltpu.VMEM((2, *shape, LANE), dtype)

        def sems(*shape):
            return pltpu.SemaphoreType.DMA((2, 2, *shape))

        r1, ways = self.half1 + (self.h1 - 1) * self.u1, len(WAYS)
        return [
            twice(ways, r1),
            twice(self.pad1, dtype=F32),
            twice(self.pad1),
            twice(self.n2, self.u2),
            twice(self.pad2, dtype=F32),
            twice(self.pad2),
            twice(self.n3, self.u3),
            twice(self.pad2),
            twice(self.pad1),
            pltpu.VMEM((self.slots, ROWS, LANE), BF),
            sems(ways, self.h1),
            sems(self.n2),
            sems(self.n3),
            sems(self.n3),
            sems(self.n2),
            sems(ways, self.h1),
            sems(),
        ]

    def bind(self, refs, g_ref, number, me, out):
        (self.r1, self.s1, self.t2, self.r2, self.s2, self.t3, self.r3, self.o3, self.o2, self.o,
         self.q1, self.q2, self.q3, self.a3, self.a2, self.a1, self.qo) = refs
        self.g, self.number, self.out, self.me = g_ref, number, out, me
        self.p = self.p1, self.p2, self.p3 = [place(me, d) for d in self.dims]

    def peer(self, k, off):
        d, n = self.dims[k], self.n[k]
        return {"dp": self.me + (lax.rem(self.p[k] + off + n, n) - self.p[k]) * STRIDE[d]}

    def zero(self):
        for ref in (self.s1, self.s2):
            ref[...] = jnp.zeros_like(ref)

    def _ring(self, k, src, dst, sems, par, way, step):
        return pltpu.make_async_remote_copy(src, dst, sems.at[0, par, way, step], sems.at[1, par, way, step],
                                            device_id=self.peer(k, turn(way)), device_id_type=MESH)

    def _span(self, halved, t, way, u, half):
        first, size = (0, u) if not halved else (0, half) if way == UP else (half, u - half)
        return first, size, max(half + (t - 2) * u, 0) if t > 1 else 0

    def rs1(self, t, way, gs, par):
        n, u = self.n1, self.u1
        dest = lax.rem(self.p1 + turn(way) * (self.h1 + 1 - t) + n, n)
        first, size, at = self._span(t == 1, t, way, u, self.half1)
        return self._ring(FIRST, self.g.at[gs, self.number, near(dest * u + first, size)], self.r1.at[par, way, pl.ds(at, size)], self.q1, par, way, t - 1)

    def _scatter(self, k, src, dst, u, sems, par):
        return [pltpu.make_async_remote_copy(src.at[par, near(lax.rem(self.p[k] + off, self.n[k]) * u, u)], dst.at[par, off], sems.at[0, par, off],
                                             sems.at[1, par, off], device_id=self.peer(k, off), device_id_type=MESH) for off in range(1, self.n[k])]

    def _gather(self, k, ref, u, sems, par):
        mine = ref.at[par, near(self.p[k] * u, u)]
        return [pltpu.make_async_remote_copy(mine, mine, sems.at[0, par, off], sems.at[1, par, off], device_id=self.peer(k, off),
                                             device_id_type=MESH) for off in range(1, self.n[k])]

    def _arrived(self, k, whole, came, u, par):
        total = whole[par, near(self.p[k] * u, u), :]
        for off in range(1, self.n[k]):
            total = total + came[par, off].astype(F32)
        return total

    def rs2(self, par):
        return self._scatter(SECOND, self.t2, self.r2, self.u2, self.q2, par)

    def rs3(self, par):
        return self._scatter(THIRD, self.t3, self.r3, self.u3, self.q3, par)

    def ag3(self, par):
        return self._gather(THIRD, self.o3, self.u3, self.a3, par)

    def ag2(self, par):
        return self._gather(SECOND, self.o2, self.u2, self.a2, par)

    def _ag(self, k, t, way, par, ref, u, half, h, sems):
        n = self.n[k]
        piece = lax.rem(self.p[k] - turn(way) * (t - 1) + n, n)
        first, size, _ = self._span(t == h, t, way, u, half)
        here = ref.at[near(piece * u + first, size)]
        return self._ring(k, here, here, sems, par, way, t - 1)

    def ag1(self, t, par, os):
        return [self._ag(FIRST, t, way, par, self.o.at[os], self.u1, self.half1, self.h1, self.a1) for way in WAYS]

    def output(self, c, os, act):
        for half in range(2):
            def go(to):
                act([pltpu.make_async_copy(self.o.at[os, pl.ds(half * D, D)], to, self.qo.at[lax.rem(c, 2), half])])

            at = self.number * 2 + half

            @pl.when(c < MLP)
            def _():
                down, *across = self.out[:-1]
                go(across[self.number - 1].at[:, near(c * STEP + half * LANE, LANE)] if self.number else down.at[c, half])

            @pl.when(c >= MLP)
            def _():
                go(self.out[-1].at[:, near(((c - MLP) * 6 + at) * LANE, LANE)])

    def event(self, e, c, squares):
        par, gs, os = lax.rem(c, 2), lax.rem(c, GS), lax.rem(c, self.slots)
        h1, f32, bf = self.h1, F32, BF
        if e <= h1:
            if e > 0:
                wait(self.rs1(e, way, gs, par) for way in WAYS)
            if e < h1:
                for way in WAYS:
                    if e > 0:
                        n, h, u, half = self.n1, self.h1, self.u1, self.half1
                        first, many, came = self._span(e == 1, e, way, u, half)
                        dest = lax.rem(self.p1 + turn(way) * (h - e) + n, n)
                        into = near(dest * u + first, many)
                        self.g[gs, self.number, into, :] = (self.g[gs, self.number, into, :].astype(f32) + self.r1[par, way, came:came + many, :].astype(f32)).astype(bf)
                    self.rs1(e + 1, way, gs, par).start()
                return
            u = self.u1
            _, _, at = self._span(False, h1, UP, u, self.half1)
            self.s1[par, :u, :] = (self.g[gs, self.number, near(self.p1 * u, u), :].astype(f32) + self.r1[par, 0, at:at + u, :].astype(f32)
                                   + self.r1[par, 1, at:at + u, :].astype(f32))
            self.t2[par] = self.s1[par].astype(bf)
            start(self.rs2(par))
        elif e == h1 + 1:
            wait(self.rs2(par))
            self.s2[par, : self.u2, :] = self._arrived(SECOND, self.s1, self.r2, self.u2, par)
            self.t3[par] = self.s2[par].astype(bf)
            start(self.rs3(par))
        elif e == h1 + 2:
            wait(self.rs3(par))
            whole = self._arrived(THIRD, self.s2, self.r3, self.u3, par).astype(bf)
            self.o3[par, near(self.p3 * self.u3, self.u3), :] = whole
            wide = whole.astype(f32)
            squares[self.number] = squares[self.number] + wide * wide
            start(self.ag3(par))
        elif e == h1 + 3:
            wait(self.ag3(par))
            self.o2[par, near(self.p2 * self.u2, self.u2), :] = self.o3[par, : self.u2, :]
            start(self.ag2(par))
        else:
            t = e - (h1 + 4)
            if t == 0:
                wait(self.ag2(par))
                self.o[os, near(self.p1 * self.u1, self.u1), :] = self.o2[par, :self.u1, :]
            elif t <= h1:
                wait(self.ag1(t, par, os))
            if t < h1:
                start(self.ag1(t + 1, par, os))
            elif t == h1:
                self.output(c, os, start)
            else:
                self.output(c, os, wait)


def barrier(me):
    sem = pltpu.get_barrier_semaphore()
    count = 0
    for d in "xyz":
        p = place(me, d)
        for off in range(1, SIZE[d]):
            other = me + (lax.rem(p + off, SIZE[d]) - p) * STRIDE[d]
            pl.semaphore_signal(sem, inc=1, device_id={"dp": other}, device_id_type=MESH)
            count += 1
    pl.semaphore_wait(sem, count)


LAST = MLP + HEADS + 1
SENT = (MLP + 1, MLP + 6, LAST + 1)
BLOCKS = MLP + 3
PER, SPACING = 4, 3
SQUARES = SENT[2] + 3
ROUNDS = SENT[2] + 7


def started(m):
    return jnp.minimum(m - 1, MLP) + m // SENT[1] + m // SENT[2], (m >= 1) & ((m <= SENT[0]) | (m == SENT[1]) | (m == SENT[2]))


def poll(colours, squares, i, j):
    for colour in colours:
        for e in range(colour.last + 2):
            if (SPACING * e - j) % PER == 0:
                block, there = started(i - (SPACING * e - j) // PER)
                if colour.number == 2:
                    there &= block < BLOCKS - 1

                @pl.when(there)
                def _():
                    colour.event(e, block, squares)


def exchange(j, mine, came, sems, me):
    def copies(dim):
        p, n = place(me, dim), SIZE[dim]
        for off in range(1, n):
            there = lax.rem(p + off, n)
            at = "zyx".index(dim)
            yield pltpu.make_async_remote_copy(mine, came.at[at, p], sems.at[0, at, off], sems.at[1, at, off],
                                               device_id={"dp": me + (there - p) * STRIDE[dim]}, device_id_type=MESH)

    if j > 0:
        dim = "zyx"[j - 1]
        for copy in copies(dim):
            copy.wait()
        came[j - 1, place(me, dim)] = mine[...]
        total = came[j - 1, 0]
        for n in range(1, SIZE[dim]):
            total = total + came[j - 1, n]
        mine[...] = total
    if j < 3:
        for copy in copies("zyx"[j]):
            copy.start()


def stage(dgu, t, n):
    k = t % 2 * HEADS + n
    return dgu.at[pl.ds(k % 4 * TILE, TILE), pl.ds(k // 4 * LANE, LANE)]


def middle_tile(t, slot, x1, x2, x3, x4, dgu, xs, hs, wo):
    att = jnp.concatenate([stage(dgu, slot, n)[...] for n in range(HEADS)], 1)
    h = (xs[slot].astype(F32) + dot(att, wo[...]).astype(BF).astype(F32)).astype(BF)
    hs[rows(t * TILE, TILE), :] = h
    b, _ = normed(h)
    at = [rows(n * TOKENS + t * TILE, TILE) for n in range(HEADS)]
    for a, part in zip(at, columns(b)):
        x1[a, :] = part
    dy = jnp.concatenate([x3[a, :] for a in at], 1)
    for ref, a in ((x2, b), (x4, dy)):
        for n, part in enumerate(columns(a.T)):
            ref[pl.ds(pl.multiple_of(t * (TILE // LANE * D) + n * D, LANE), D), :] = part


def mlp_tile(t, x1, x3, wg, wu, wd, ff, dgu):
    at = [pl.ds(n * TOKENS + t * WIDE, WIDE) for n in range(HEADS)]
    b = jnp.concatenate([x1[a, :] for a in at], 1)
    dy = jnp.concatenate([x3[a, :] for a in at], 1)
    gate, upper = dot(b, wg[...]), dot(b, wu[...])
    by_f = dot_t(dy, wd[...]).astype(BF).astype(F32)
    gain = 1 / (1 + jnp.exp(-gate))
    act = gate * gain
    here = pl.ds(t * WIDE, WIDE)
    ff[here, :] = (act * upper).astype(BF)
    dgu[here, :STEP] = (by_f * upper * (gain * (1 + gate * (1 - gain)))).astype(BF)
    dgu[here, STEP:] = (by_f * act).astype(BF)


def add_input_gradient(t, wg, wu, dgu, db):
    here = rows(t * WIDE, WIDE)
    part = dot_t(dgu[here, :], jnp.concatenate([wg[...], wu[...]], 1))
    for n, column in enumerate(columns(part)):
        at = rows(n * TOKENS + t * WIDE, WIDE)
        db[at, :] = db[at, :] + column


def turned_block(ref):
    return jnp.concatenate([ref[n * D : (n + 1) * D, :] for n in range(CHUNKS)], 1)


def put(g, slot, colour, half, w):
    for n, column in enumerate(columns(w)):
        g[slot, colour, (half + n) * D : (half + n + 1) * D, :] = column.astype(BF)


def residual_tile(t, x1, x3, x4, db, hs, wo, delta):
    at = [rows(n * TOKENS + t * TILE, TILE) for n in range(HEADS)]
    by_b = jnp.concatenate([db[a, :] for a in at], 1).astype(BF).astype(F32)
    h = hs[t * TILE : (t + 1) * TILE, :]
    wide = h.astype(F32)
    _, scale = normed(h)
    by_h = (scale * by_b - wide * (scale * scale * scale * jnp.mean(by_b * wide, -1, keepdims=True))).astype(BF)
    by_h = (by_h.astype(F32) + jnp.concatenate([x3[a, :] for a in at], 1).astype(F32)).astype(BF)
    for a, column in zip(at, columns(by_h)):
        x3[a, :] = column
    by_att = dot_t(by_h, wo[...]).astype(BF)
    for n, column in enumerate(columns(by_att)):
        delta[n : n + 1, t * TILE : (t + 1) * TILE] = jnp.sum((column.astype(F32) * x1[at[n], :].astype(F32)).T, 0, keepdims=True)
        x4[at[n], :] = column


def attention_block(head, first, key, many, strips, edge, x1, x4, k, v, db, dq, lse, delta):
    kk, vv = k[rows(key, many), :], v[rows(key, many), :]
    at = [rows(head * TOKENS + first + s, STRIP) for s in strips]
    qs, dos = [x1[a, :] for a in at], [x4[a, :] for a in at]
    scores, dps = [dot_t(kk, q) for q in qs], [dot_t(vv, d) for d in dos]
    dk = dv = None
    for n, s in enumerate(strips):
        here = pl.ds(first + s, STRIP)
        p = jnp.exp2(scores[n] * E - lse[pl.ds(head, 1), here] * (E / SCALE))
        if edge and n == 0:
            shape = (STRIP, STRIP)
            p = jnp.where(lax.broadcasted_iota(jnp.int32, shape, 1) >= lax.broadcasted_iota(jnp.int32, shape, 0), p, 0.0)
        ds = (p * (dps[n] - delta[pl.ds(head, 1), here])).astype(BF)
        a, b = dot(p.astype(BF), dos[n]), dot(ds, qs[n])
        dv, dk = (a, b) if dv is None else (dv + a, dk + b)
        dq[:, s : s + STRIP] += dot(kk.T, ds)
    for base, part in ((0, dk), (TOKENS, dv)):
        db[pl.ds(pl.multiple_of(base + key, STRIP), many), :] += part


def turn_back(t, first, cos, sin):
    here = pl.ds(first, t.shape[0])
    t = t.astype(BF).astype(F32)
    return (t * cos[here, :] - pltpu.roll(t, HALF, 1) * sin[here, :]).astype(BF)


def backward_kernel(x_hbm, dy_hbm, att_hbm, attt_hbm, q_hbm, k_hbm, v_hbm, at_hbm, lse_hbm, cos_hbm, sin_hbm, wg_hbm, wu_hbm, wd_hbm, wo_hbm,
                    gd_hbm, gg_hbm, gu_hbm, ga_hbm, sq_hbm,
                    x1, x2, x3, x4, db, ff, dgu, wg, wu, wd, g, k, v, lse, delta, cos, sin, wo, xs, hs, dq, squares, total, came,
                    sem_x, sem_w, sem_in, sem_t, sem_sq, *rest):
    me = lax.axis_index("dp")
    barrier(me)
    colours, at = [Colour(dims) for dims in COLOURS], 0
    for number, colour in enumerate(colours):
        many = len(colour.scratch())
        colour.bind(rest[at : at + many], g, number, me, (gd_hbm, gg_hbm, gu_hbm, ga_hbm))
        at += many

    def load(src, dst, sem):
        return pltpu.make_async_copy(src, dst, sem)

    dys = [load(dy_hbm.at[0, :, pl.ds(n * LANE, LANE)], x3.at[pl.ds(n * TOKENS, TOKENS)], sem_x.at[n]) for n in range(HEADS)]
    first = load(wo_hbm.at[0], wo, sem_x.at[HEADS])
    later = [load(src, dst, sem_in.at[n]) for n, (src, dst) in enumerate(((k_hbm, k), (v_hbm, v), (lse_hbm, lse), (cos_hbm, cos), (sin_hbm, sin)))]
    swaps = [load(src, dst, sem_x.at[n]) for n, (src, dst) in enumerate(((att_hbm, x1), (attt_hbm, x2), (q_hbm, x1), (at_hbm, x2)))]

    def weights(i):
        par, cols = lax.rem(i, 2), rows(i * STEP, STEP)
        return [load(src, dst.at[par], sem_w.at[par, n]) for n, (src, dst) in enumerate(
            ((wg_hbm.at[0, :, cols], wg), (wu_hbm.at[0, :, cols], wu), (wd_hbm.at[0, cols, :], wd)))]

    def tile(t, slot):
        here = rows(t * TILE, TILE)
        heads = [load(att_hbm.at[pl.ds(n * TOKENS + pl.multiple_of(t * TILE, TILE), TILE)], stage(dgu, slot, n), sem_t.at[slot, n]) for n in range(HEADS)]
        return heads + [load(x_hbm.at[0, here], xs.at[slot], sem_t.at[slot, HEADS])]

    for copies in ([first], tile(0, 0), dys, tile(1, 1), weights(0), later):
        start(copies)
    db[...] = jnp.zeros_like(db)
    squares[...] = jnp.zeros_like(squares)
    for colour in colours:
        colour.zero()
    wait([first] + dys)

    def middle(n, _):
        for slot in range(2):
            t = 2 * n + slot
            wait(tile(t, slot))
            middle_tile(t, slot, x1, x2, x3, x4, dgu, xs, hs, wo)

            @pl.when(n == 0)
            def _():
                start(tile(t + 2, slot))

    lax.fori_loop(0, 2, middle, None)

    def body(i, _):
        par = lax.rem(i, 2)
        busy = (wg.at[par], wu.at[par], wd.at[par])

        def part(j):
            poll(colours, squares, i, j)

            @pl.when(i < MLP)
            def _():
                if j == 0:
                    wait(weights(i))

                    @pl.when(i + 1 < MLP)
                    def _():
                        start(weights(i + 1))

                if j < 2:
                    mlp_tile(j, x1, x3, *busy, ff, dgu)
                elif j == 2:
                    @pl.when(i == MLP - 1)
                    def _():
                        swaps[0].start()

                    def half(t, _):
                        add_input_gradient(t, busy[0], busy[1], dgu, db)
                    lax.fori_loop(0, 2, half, None)
                else:
                    slot = lax.rem(i, GS)
                    put(g, slot, 0, 0, dot(turned_block(x4), ff[...]))
                    put(g, slot, 1, 0, dot(turned_block(x2), dgu[:, :STEP]))
                    put(g, slot, 2, 0, dot(turned_block(x2), dgu[:, STEP:]))

            @pl.when(i == MLP)
            def _():
                if j == 0:
                    swaps[1].start()
                    swaps[0].wait()
                    wait(later)
                if j < 2:
                    for t in (2 * j, 2 * j + 1):
                        residual_tile(t, x1, x3, x4, db, hs, wo, delta)
                elif j == 2:
                    swaps[2].start()
                    swaps[1].wait()
                    db[: 2 * TOKENS, :] = jnp.zeros((2 * TOKENS, LANE), F32)
                if j >= 2:
                    def by_wo(n):
                        return dot(turned_block(x2), jnp.concatenate([x3[m * TOKENS : (m + 1) * TOKENS, :] for m in range(n, min(n + 2, HEADS))], 1))
                    for n in ((0, 2), (4, 6))[j - 2]:
                        put(g, (MLP + n // 6) % GS, (n // 2) % 3, 0, by_wo(n))
                if j == 3:
                    swaps[3].start()
                    swaps[2].wait()

            head = i - MLP - 1

            @pl.when((head >= 0) & (head < HEADS))
            def _():
                refs = (x1, x4, k, v, db, dq, lse, delta)
                late = WIDE if j in (1, 2) else 0
                if j < 2:
                    dq[...] = jnp.zeros_like(dq)
                if j == 1:
                    def seen(n, _):
                        attention_block(head, WIDE, n * TILE, TILE, range(0, WIDE, STRIP), False, *refs)
                    lax.fori_loop(0, 2, seen, None)
                if j in (0, 2):
                    for key in range(0, WIDE, STRIP):
                        attention_block(head, late, late + key, STRIP, range(key, WIDE, STRIP), True, *refs)
                    x3[rows(head * TOKENS + late, WIDE), :] = turn_back((dq[...] * SCALE).T, late, cos, sin)
                if j == 3:
                    @pl.when(head == 0)
                    def _():
                        swaps[3].wait()

                    def by_wq(n, many):
                        return dot(turned_block(x2), jnp.concatenate([x3[m * TOKENS : (m + 1) * TOKENS, :] for m in range(n, n + many)], 1))

                    for n in range(0, HEADS, 2):
                        @pl.when(head == n)
                        def _():
                            block = MLP + 1 + n // 6
                            if n == 0:
                                put(g, block % GS, 0, 1, by_wq(0, 1))
                            else:
                                put(g, block % GS, (n // 2) % 3, 0, by_wq(n - 1, 2))

            @pl.when(i == LAST)
            def _():
                if j < 2:
                    part = db[j * TOKENS : (j + 1) * TOKENS, :]
                    x1[j * TOKENS : (j + 1) * TOKENS, :] = part.astype(BF) if j else turn_back(part * SCALE, 0, cos, sin)
                elif j == 2:
                    both = jnp.concatenate([x1[:TOKENS, :], x1[TOKENS : 2 * TOKENS, :]], 1)
                    put(g, (BLOCKS - 1) % GS, 1, 0, dot(turned_block(x2), both))

            if j == 0:
                for step in range(4):
                    @pl.when(i == SQUARES + step)
                    def _():
                        if step == 0:
                            wide = squares[0] + squares[1] + squares[2]
                            total[...] = wide[:8, :] + wide[8:, :]
                        exchange(step, total, came, sem_sq, me)

        for j in range(PER):
            part(j)
        return None

    lax.fori_loop(0, ROUNDS, body, None)
    copy = load(total, sq_hbm, sem_in.at[0])
    copy.start()
    copy.wait()


def backward(args):
    flat = pltpu.VMEM((FLAT, LANE), BF)
    narrow = pltpu.VMEM((TOKENS, LANE), BF)
    table, heads = pltpu.VMEM((TOKENS, LANE), F32), pltpu.VMEM((HEADS, TOKENS), F32)
    sem = pltpu.SemaphoreType.DMA
    thirds = len(COLOURS)
    return pl.pallas_call(
        backward_kernel,
        in_specs=[ANY] * len(args),
        out_specs=[ANY] * 5,
        out_shape=[like(MLP, 2, D, LANE), like(D, FF), like(D, FF), like(D, 6 * thirds * LANE), like(8, LANE, dtype=F32)],
        scratch_shapes=[flat] * 4
        + [pltpu.VMEM((FLAT, LANE), F32), pltpu.VMEM((TOKENS, STEP), BF), pltpu.VMEM((TOKENS, 2 * STEP), BF)]
        + [pltpu.VMEM((2, D, STEP), BF)] * 2
        + [pltpu.VMEM((2, STEP, D), BF), pltpu.VMEM((GS, thirds, ROWS, LANE), BF), narrow, narrow, heads, heads, table, table]
        + [pltpu.VMEM((D, D), BF), pltpu.VMEM((2, TILE, D), BF), pltpu.VMEM((TOKENS, D), BF), pltpu.VMEM((LANE, WIDE), F32)]
        + [pltpu.VMEM((thirds, 16, LANE), F32), pltpu.VMEM((8, LANE), F32), pltpu.VMEM((thirds, 8, 8, LANE), F32)]
        + [sem((HEADS + 1,)), sem((2, thirds)), sem((5,)), sem((2, HEADS + 1)), sem((2, thirds, 8))]
        + [s for dims in COLOURS for s in Colour(dims).scratch()],
        compiler_params=pltpu.CompilerParams(collective_id=0, has_side_effects=True, vmem_limit_bytes=63 * MIB),
        cost_estimate=cost(16 * TOKENS * D * FF, 120),
    )(*args)


def adamw(w, m, v, new_w, new_m, new_v, g):
    m = 0.9 * m[0] + 0.1 * g
    v = 0.95 * v[0] + 0.05 * g * g
    wide = w[0].astype(F32)
    new_w[0] = (wide - 0.02 * (m * lax.rsqrt(v + 1e-8) + 0.1 * wide)).astype(BF)
    new_m[0], new_v[0] = m, v


def update_kernel(count, sq_ref, *refs):
    total = jnp.sum(jnp.sum(sq_ref[...], 0, keepdims=True), 1, keepdims=True)
    factor = jnp.minimum(1.0, 0.5 * lax.rsqrt(total / count + 1e-30))
    names = len(refs) // 7
    for k, ref in enumerate(refs[:names]):
        g = ref[...] if len(ref.shape) == 2 else jnp.concatenate([ref[0, half].T for half in range(2)])
        adamw(*refs[names + k :: names], g.astype(F32) * factor)


def update(steps, gs, gradients, blocks, sq, arrays, count):
    return pl.pallas_call(
        functools.partial(update_kernel, count),
        grid=(steps,),
        in_specs=[whole((8, LANE))] + gradients + blocks * 3,
        out_specs=blocks * 3,
        out_shape=[like(*a.shape, dtype=a.dtype) for a in arrays],
        compiler_params=ROOM,
    )(sq, *gs, *arrays)


IN_MLP, IN_ATTENTION = ("w_down", "w_gate", "w_up"), ("wo", "wq", "wk", "wv")
STEPS_REST = 4
REST = D // STEPS_REST


def down(shape):
    return pl.BlockSpec((1, *shape), lambda i: (0, i, 0))


def across(shape, col=None):
    return pl.BlockSpec(shape, (lambda i: (0,) * (len(shape) - 1) + (i,)) if col is None else lambda i: (i, col))


NAMES = ("wq", "wk", "wv", "wo", "w_gate", "w_up", "w_down")


def solution(mesh):
    def step(x, dy, *arrays):
        kinds = [dict(zip(NAMES, arrays[n : n + len(NAMES)])) for n in range(0, len(arrays), len(NAMES))]
        w = kinds[0]
        cos, sin = tables()
        q, k, v, at = project(x, w["wq"], w["wk"], w["wv"], cos, sin)
        att, attt, lse = attend(q, k, v)
        flat = lambda a: a.reshape(FLAT, LANE)
        *gs, sq = backward((x, dy, flat(att), flat(attt), flat(q), k, v, flat(at), lse, cos, sin, w["w_gate"], w["w_up"], w["w_down"], w["wo"]))
        count, new = sum(a.size for a in w.values()), {}
        third = across((D, STEP))
        for names, *rest in (
            (IN_MLP, MLP, gs[:3], [pl.BlockSpec((1, 2, D, LANE), lambda i: (i, 0, 0, 0)), third, third],
             [down((STEP, D))] + [across((1, D, STEP))] * 2),
            (IN_ATTENTION, STEPS_REST, gs[3:] * 4, [across((REST, D), n) for n in range(2)] + [across((REST, LANE), n) for n in (2 * HEADS, 2 * HEADS + 1)],
             [down((REST, D))] * 2 + [down((REST, LANE))] * 2),
        ):
            done = update(*rest, sq, [kind[name] for kind in kinds for name in names], count)
            new.update(zip([(n, name) for n in range(len(kinds)) for name in names], done))
        return tuple(new[n, name] for n in range(len(kinds)) for name in NAMES)

    states, all_of, ours = P(("rep", "dp"), None, None), P(None, None, None), P("rep", None, None)
    many = 3 * len(NAMES)
    return jax.shard_map(step, mesh=mesh, in_specs=(states, states) + (all_of,) * many, out_specs=(ours,) * many, check_vma=False)
```

```python
import functools

import jax
import jax.numpy as jnp
import numpy as np
from jax import lax
from jax.experimental import pallas as pl
from jax.experimental.pallas import tpu as pltpu
from jax.sharding import PartitionSpec as P

BF, F32 = jnp.bfloat16, jnp.float32
MESH = pl.DeviceIdType.MESH
ANY = pl.BlockSpec(memory_space=pl.ANY)
LANE, HALF = 128, 64
D, HEADS, FF, TOKENS = 896, 7, 2560, 2048
THETA = 10000
TILE = 512
WIDE, STRIP = 1024, 256
CHUNKS = TOKENS // LANE
FLAT = HEADS * TOKENS
STEP = 256
MLP = FF // STEP
TINY = 1e-6
SCALE = LANE**-0.5
E = SCALE * 1.4426950408889634
NEG = -1e30
MIB = 2**20


def dot(a, b, ca=1, cb=0):
    return lax.dot_general(a, b, (((ca,), (cb,)), ((), ())), preferred_element_type=F32)


def normed(h):
    wide = h.astype(F32)
    scale = lax.rsqrt(jnp.mean(wide * wide, -1, keepdims=True) + TINY)
    return (wide * scale).astype(BF), scale


def dot_t(a, b):
    return dot(a, b, 1, 1)


def columns(a):
    return [a[:, n : n + LANE] for n in range(0, a.shape[1], LANE)]


def rows(start, size):
    return pl.ds(start if isinstance(start, int) else pl.multiple_of(start, size), size)


def tables():
    angle = np.arange(TOKENS, dtype=np.float64)[:, None] * THETA ** (-np.arange(HALF, dtype=np.float64) / HALF)
    cos, sin = np.cos(angle), np.sin(angle)
    return jnp.asarray(np.concatenate([cos, cos], 1), F32), jnp.asarray(np.concatenate([-sin, sin], 1), F32)


def project_kernel(x_ref, cos_ref, sin_ref, wq_ref, wk_ref, wv_ref, q_ref, k_ref, v_ref, at_ref):
    a, _ = normed(x_ref[0])
    for n, part in enumerate(columns(a.T)):
        at_ref[n] = part

    def turned(t):
        t = t.astype(BF).astype(F32)
        return (t * cos_ref[...] + pltpu.roll(t, HALF, 1) * sin_ref[...]).astype(BF)

    for n, part in enumerate(columns(dot(a, wq_ref[0]))):
        q_ref[n] = turned(part)
    k_ref[...] = turned(dot(a, wk_ref[0]))
    v_ref[...] = dot(a, wv_ref[0]).astype(BF)


def cost(flops, megabytes):
    return pl.CostEstimate(flops=flops, bytes_accessed=megabytes * MIB, transcendentals=0)


def like(*shape, dtype=BF):
    return jax.ShapeDtypeStruct(shape, dtype)


def whole(shape):
    return pl.BlockSpec(shape, lambda i: (0,) * len(shape))


TILES = pl.BlockSpec((1, TILE, D), lambda i: (0, i, 0))
NARROW = pl.BlockSpec((TILE, LANE), lambda i: (i, 0))
SPLIT = pl.BlockSpec((HEADS, TILE, LANE), lambda i: (0, i, 0))
TURNED = pl.BlockSpec((TILE // LANE, D, LANE), lambda i: (i, 0, 0))
ROOM = pltpu.CompilerParams(vmem_limit_bytes=63 * MIB)
STEPS = (TOKENS // TILE,)


def project(x, wq, wk, wv, cos, sin):
    return pl.pallas_call(
        project_kernel,
        grid=STEPS,
        in_specs=[TILES, NARROW, NARROW, whole((1, D, D)), whole((1, D, LANE)), whole((1, D, LANE))],
        out_specs=[SPLIT, NARROW, NARROW, TURNED],
        out_shape=[like(HEADS, TOKENS, LANE), like(TOKENS, LANE), like(TOKENS, LANE), like(CHUNKS, D, LANE)],
        compiler_params=ROOM,
        cost_estimate=cost(2 * TOKENS * D * (D + 2 * LANE), 12),
    )(x, cos, sin, wq, wk, wv)


def attend_kernel(q_ref, k_ref, v_ref, o_ref, ot_ref, lse_ref, top_s, mix_s):
    iq = pl.program_id(0)
    top_s[...] = jnp.full_like(top_s, NEG)
    mix_s[...] = jnp.zeros_like(mix_s)

    def block(first, many, strips, edge):
        here, wide = pl.ds(first, many), TILE // 2 if edge else TILE
        pieces = [(n, s) for n in range(HEADS) for s in strips]
        keys = k_ref[here, :]
        scores = [dot_t(keys, q_ref[n, s : s + wide, :]) for n, s in pieces]
        weights, keeps = [], []
        for (n, s), score in zip(pieces, scores):
            if edge and s == strips[0]:
                shape = (many, wide)
                score = jnp.where(lax.broadcasted_iota(jnp.int32, shape, 1) >= lax.broadcasted_iota(jnp.int32, shape, 0), score, 2 * NEG)
            old = top_s[n : n + 1, s : s + wide]
            top = jnp.maximum(old, score.max(axis=0, keepdims=True))
            top_s[n : n + 1, s : s + wide] = top
            weights.append(jnp.exp2((score - top) * E).astype(BF))
            keeps.append(jnp.exp2((old - top) * E))
        values = jnp.concatenate([v_ref[here, :].T, jnp.ones((8, many), BF)], axis=0)
        for (n, s), p, keep in zip(pieces, weights, keeps):
            mix_s[n, :, s : s + wide] = mix_s[n, :, s : s + wide] * keep + dot(values, p)

    lax.fori_loop(0, iq, lambda j, _: block(pl.multiple_of(j * TILE, TILE), TILE, (0,), False), None)
    for s in (0, STRIP):
        block(pl.multiple_of(iq * TILE + s, STRIP), STRIP, range(s, TILE, STRIP), True)
    for n in range(HEADS):
        total = mix_s[n, LANE : LANE + 1, :]
        out = (mix_s[n, :LANE, :] * (1 / total)).astype(BF)
        o_ref[n] = out.T
        for m, part in enumerate(columns(out)):
            ot_ref[m, n * LANE : (n + 1) * LANE, :] = part
        lse_ref[n : n + 1, :] = top_s[n : n + 1, :] * SCALE + jnp.log(total)


def attend(q, k, v):
    return pl.pallas_call(
        attend_kernel,
        grid=STEPS,
        in_specs=[SPLIT, whole((TOKENS, LANE)), whole((TOKENS, LANE))],
        out_specs=[SPLIT, TURNED, pl.BlockSpec((HEADS, TILE), lambda i: (0, i))],
        out_shape=[like(HEADS, TOKENS, LANE), like(CHUNKS, D, LANE), like(HEADS, TOKENS, dtype=F32)],
        scratch_shapes=[pltpu.VMEM((HEADS, TILE), F32), pltpu.VMEM((HEADS, LANE + 8, TILE), F32)],
        compiler_params=ROOM,
        cost_estimate=cost(4 * HEADS * TOKENS * TOKENS * LANE, 8),
    )(q, k, v)


ROWS = 1792
SIZE = {"x": 4, "y": 4, "z": 8}
STRIDE = {"x": 32, "y": 8, "z": 1}
COLOURS = ("xyz", "yxz", "zxy")
GS = 4


def up(n, m):
    return -(-n // m) * m


FIRST, SECOND, THIRD = range(3)
WAYS = 0, 1
UP, DOWN = WAYS


def place(me, dim):
    return (me // STRIDE[dim]) % SIZE[dim]


def turn(way):
    return 1 - 2 * way


def near(first, size):
    return pl.ds(pl.multiple_of(first, LANE if size == LANE else 16), size)


def start(copies):
    for copy in copies:
        copy.start()


def wait(copies):
    for copy in copies:
        copy.wait()


class Colour:
    def __init__(self, dims):
        self.dims = dims
        self.n = self.n1, self.n2, self.n3 = [SIZE[d] for d in dims]
        self.u1 = ROWS // self.n1
        self.pad1 = up(self.u1, self.n2 * 16)
        self.u2 = self.pad1 // self.n2
        self.pad2 = up(self.u2, self.n3 * 16)
        self.u3 = self.pad2 // self.n3
        self.h1 = self.n1 // 2
        self.half1 = up(self.u1 // 2, 16)
        self.slots = 3 + self.h1 // 2
        self.last = 2 * self.h1 + 4

    def scratch(self):
        def twice(*shape, dtype=BF):
            return pltpu.VMEM((2, *shape, LANE), dtype)

        def sems(*shape):
            return pltpu.SemaphoreType.DMA((2, 2, *shape))

        r1, ways = self.half1 + (self.h1 - 1) * self.u1, len(WAYS)
        return [
            twice(ways, r1),
            twice(self.pad1, dtype=F32),
            twice(self.pad1),
            twice(self.n2, self.u2),
            twice(self.pad2, dtype=F32),
            twice(self.pad2),
            twice(self.n3, self.u3),
            twice(self.pad2),
            twice(self.pad1),
            pltpu.VMEM((self.slots, ROWS, LANE), BF),
            sems(ways, self.h1),
            sems(self.n2),
            sems(self.n3),
            sems(self.n3),
            sems(self.n2),
            sems(ways, self.h1),
            sems(),
        ]

    def bind(self, refs, g_ref, number, me, out):
        (self.r1, self.s1, self.t2, self.r2, self.s2, self.t3, self.r3, self.o3, self.o2, self.o,
         self.q1, self.q2, self.q3, self.a3, self.a2, self.a1, self.qo) = refs
        self.g, self.number, self.out, self.me = g_ref, number, out, me
        self.p = self.p1, self.p2, self.p3 = [place(me, d) for d in self.dims]

    def peer(self, k, off):
        d, n = self.dims[k], self.n[k]
        return {"dp": self.me + (lax.rem(self.p[k] + off + n, n) - self.p[k]) * STRIDE[d]}

    def zero(self):
        for ref in (self.s1, self.s2):
            ref[...] = jnp.zeros_like(ref)

    def _ring(self, k, src, dst, sems, par, way, step):
        return pltpu.make_async_remote_copy(src, dst, sems.at[0, par, way, step], sems.at[1, par, way, step],
                                            device_id=self.peer(k, turn(way)), device_id_type=MESH)

    def _span(self, halved, t, way, u, half):
        first, size = (0, u) if not halved else (0, half) if way == UP else (half, u - half)
        return first, size, max(half + (t - 2) * u, 0) if t > 1 else 0

    def rs1(self, t, way, gs, par):
        n, u = self.n1, self.u1
        dest = lax.rem(self.p1 + turn(way) * (self.h1 + 1 - t) + n, n)
        first, size, at = self._span(t == 1, t, way, u, self.half1)
        return self._ring(FIRST, self.g.at[gs, self.number, near(dest * u + first, size)], self.r1.at[par, way, pl.ds(at, size)], self.q1, par, way, t - 1)

    def _scatter(self, k, src, dst, u, sems, par):
        return [pltpu.make_async_remote_copy(src.at[par, near(lax.rem(self.p[k] + off, self.n[k]) * u, u)], dst.at[par, off], sems.at[0, par, off],
                                             sems.at[1, par, off], device_id=self.peer(k, off), device_id_type=MESH) for off in range(1, self.n[k])]

    def _gather(self, k, ref, u, sems, par):
        mine = ref.at[par, near(self.p[k] * u, u)]
        return [pltpu.make_async_remote_copy(mine, mine, sems.at[0, par, off], sems.at[1, par, off], device_id=self.peer(k, off),
                                             device_id_type=MESH) for off in range(1, self.n[k])]

    def _arrived(self, k, whole, came, u, par):
        total = whole[par, near(self.p[k] * u, u), :]
        for off in range(1, self.n[k]):
            total = total + came[par, off].astype(F32)
        return total

    def rs2(self, par):
        return self._scatter(SECOND, self.t2, self.r2, self.u2, self.q2, par)

    def rs3(self, par):
        return self._scatter(THIRD, self.t3, self.r3, self.u3, self.q3, par)

    def ag3(self, par):
        return self._gather(THIRD, self.o3, self.u3, self.a3, par)

    def ag2(self, par):
        return self._gather(SECOND, self.o2, self.u2, self.a2, par)

    def _ag(self, k, t, way, par, ref, u, half, h, sems):
        n = self.n[k]
        piece = lax.rem(self.p[k] - turn(way) * (t - 1) + n, n)
        first, size, _ = self._span(t == h, t, way, u, half)
        here = ref.at[near(piece * u + first, size)]
        return self._ring(k, here, here, sems, par, way, t - 1)

    def ag1(self, t, par, os):
        return [self._ag(FIRST, t, way, par, self.o.at[os], self.u1, self.half1, self.h1, self.a1) for way in WAYS]

    def output(self, c, os, act):
        for half in range(2):
            def go(to):
                act([pltpu.make_async_copy(self.o.at[os, pl.ds(half * D, D)], to, self.qo.at[lax.rem(c, 2), half])])

            at = self.number * 2 + half

            @pl.when(c < MLP)
            def _():
                down, *across = self.out[:-1]
                go(across[self.number - 1].at[:, near(c * STEP + half * LANE, LANE)] if self.number else down.at[c, half])

            @pl.when(c >= MLP)
            def _():
                go(self.out[-1].at[:, near(((c - MLP) * 6 + at) * LANE, LANE)])

    def event(self, e, c, squares):
        par, gs, os = lax.rem(c, 2), lax.rem(c, GS), lax.rem(c, self.slots)
        h1, f32, bf = self.h1, F32, BF
        if e <= h1:
            if e > 0:
                wait(self.rs1(e, way, gs, par) for way in WAYS)
            if e < h1:
                for way in WAYS:
                    if e > 0:
                        n, h, u, half = self.n1, self.h1, self.u1, self.half1
                        first, many, came = self._span(e == 1, e, way, u, half)
                        dest = lax.rem(self.p1 + turn(way) * (h - e) + n, n)
                        into = near(dest * u + first, many)
                        self.g[gs, self.number, into, :] = (self.g[gs, self.number, into, :].astype(f32) + self.r1[par, way, came:came + many, :].astype(f32)).astype(bf)
                    self.rs1(e + 1, way, gs, par).start()
                return
            u = self.u1
            _, _, at = self._span(False, h1, UP, u, self.half1)
            self.s1[par, :u, :] = (self.g[gs, self.number, near(self.p1 * u, u), :].astype(f32) + self.r1[par, 0, at:at + u, :].astype(f32)
                                   + self.r1[par, 1, at:at + u, :].astype(f32))
            self.t2[par] = self.s1[par].astype(bf)
            start(self.rs2(par))
        elif e == h1 + 1:
            wait(self.rs2(par))
            self.s2[par, : self.u2, :] = self._arrived(SECOND, self.s1, self.r2, self.u2, par)
            self.t3[par] = self.s2[par].astype(bf)
            start(self.rs3(par))
        elif e == h1 + 2:
            wait(self.rs3(par))
            whole = self._arrived(THIRD, self.s2, self.r3, self.u3, par).astype(bf)
            self.o3[par, near(self.p3 * self.u3, self.u3), :] = whole
            wide = whole.astype(f32)
            squares[self.number] = squares[self.number] + wide * wide
            start(self.ag3(par))
        elif e == h1 + 3:
            wait(self.ag3(par))
            self.o2[par, near(self.p2 * self.u2, self.u2), :] = self.o3[par, : self.u2, :]
            start(self.ag2(par))
        else:
            t = e - (h1 + 4)
            if t == 0:
                wait(self.ag2(par))
                self.o[os, near(self.p1 * self.u1, self.u1), :] = self.o2[par, :self.u1, :]
            elif t <= h1:
                wait(self.ag1(t, par, os))
            if t < h1:
                start(self.ag1(t + 1, par, os))
            elif t == h1:
                self.output(c, os, start)
            else:
                self.output(c, os, wait)


def barrier(me):
    sem = pltpu.get_barrier_semaphore()
    count = 0
    for d in "xyz":
        p = place(me, d)
        for off in range(1, SIZE[d]):
            other = me + (lax.rem(p + off, SIZE[d]) - p) * STRIDE[d]
            pl.semaphore_signal(sem, inc=1, device_id={"dp": other}, device_id_type=MESH)
            count += 1
    pl.semaphore_wait(sem, count)


LAST = MLP + HEADS
SENT = (MLP + 1, MLP + 6, LAST + 1)
BLOCKS = MLP + 3
PER, SPACING = 4, 3
SQUARES = SENT[2] + 3
ROUNDS = SENT[2] + 8


def started(m):
    return jnp.minimum(m - 1, MLP) + m // SENT[1] + m // SENT[2], (m >= 1) & ((m <= SENT[0]) | (m == SENT[1]) | (m == SENT[2]))


def poll(colours, squares, i, j):
    for colour in colours:
        for e in range(colour.last + 2):
            if (SPACING * e - j) % PER == 0:
                block, there = started(i - (SPACING * e - j) // PER)
                if colour.number == 2:
                    there &= block < BLOCKS - 1

                @pl.when(there)
                def _():
                    colour.event(e, block, squares)


def exchange(j, mine, came, sems, me):
    def copies(dim):
        p, n = place(me, dim), SIZE[dim]
        for off in range(1, n):
            there = lax.rem(p + off, n)
            at = "zyx".index(dim)
            yield pltpu.make_async_remote_copy(mine, came.at[at, p], sems.at[0, at, off], sems.at[1, at, off],
                                               device_id={"dp": me + (there - p) * STRIDE[dim]}, device_id_type=MESH)

    if j > 0:
        dim = "zyx"[j - 1]
        for copy in copies(dim):
            copy.wait()
        came[j - 1, place(me, dim)] = mine[...]
        total = came[j - 1, 0]
        for n in range(1, SIZE[dim]):
            total = total + came[j - 1, n]
        mine[...] = total
    if j < 3:
        for copy in copies("zyx"[j]):
            copy.start()


def stage(dgu, t, n):
    k = t % 2 * HEADS + n
    return dgu.at[pl.ds(k % 4 * TILE, TILE), pl.ds(k // 4 * LANE, LANE)]


def middle_tile(t, slot, x1, x2, x3, x4, dgu, xs, hs, wo):
    att = jnp.concatenate([stage(dgu, slot, n)[...] for n in range(HEADS)], 1)
    h = (xs[slot].astype(F32) + dot(att, wo[...]).astype(BF).astype(F32)).astype(BF)
    hs[rows(t * TILE, TILE), :] = h
    b, _ = normed(h)
    at = [rows(n * TOKENS + t * TILE, TILE) for n in range(HEADS)]
    for a, part in zip(at, columns(b)):
        x1[a, :] = part
    dy = jnp.concatenate([x3[a, :] for a in at], 1)
    for ref, a in ((x2, b), (x4, dy)):
        for n, part in enumerate(columns(a.T)):
            ref[pl.ds(pl.multiple_of(t * (TILE // LANE * D) + n * D, LANE), D), :] = part


def mlp_tile(t, x1, x3, wg, wu, wd, ff, dgu):
    at = [pl.ds(n * TOKENS + t * WIDE, WIDE) for n in range(HEADS)]
    b = jnp.concatenate([x1[a, :] for a in at], 1)
    dy = jnp.concatenate([x3[a, :] for a in at], 1)
    gate, upper = dot(b, wg[...]), dot(b, wu[...])
    by_f = dot_t(dy, wd[...]).astype(BF).astype(F32)
    gain = 1 / (1 + jnp.exp(-gate))
    act = gate * gain
    here = pl.ds(t * WIDE, WIDE)
    ff[here, :] = (act * upper).astype(BF)
    dgu[here, :STEP] = (by_f * upper * (gain * (1 + gate * (1 - gain)))).astype(BF)
    dgu[here, STEP:] = (by_f * act).astype(BF)


def add_input_gradient(t, wg, wu, dgu, db):
    here = rows(t * WIDE, WIDE)
    part = dot_t(dgu[here, :], jnp.concatenate([wg[...], wu[...]], 1))
    for n, column in enumerate(columns(part)):
        at = rows(n * TOKENS + t * WIDE, WIDE)
        db[at, :] = db[at, :] + column


def turned_block(ref):
    return jnp.concatenate([ref[n * D : (n + 1) * D, :] for n in range(CHUNKS)], 1)


def put(g, slot, colour, half, w):
    for n, column in enumerate(columns(w)):
        g[slot, colour, (half + n) * D : (half + n + 1) * D, :] = column.astype(BF)


def residual_tile(t, x1, x3, x4, db, hs, wo, delta):
    at = [rows(n * TOKENS + t * TILE, TILE) for n in range(HEADS)]
    by_b = jnp.concatenate([db[a, :] for a in at], 1).astype(BF).astype(F32)
    h = hs[t * TILE : (t + 1) * TILE, :]
    wide = h.astype(F32)
    _, scale = normed(h)
    by_h = (scale * by_b - wide * (scale * scale * scale * jnp.mean(by_b * wide, -1, keepdims=True))).astype(BF)
    by_h = (by_h.astype(F32) + jnp.concatenate([x3[a, :] for a in at], 1).astype(F32)).astype(BF)
    for a, column in zip(at, columns(by_h)):
        x3[a, :] = column
    by_att = dot_t(by_h, wo[...]).astype(BF)
    for n, column in enumerate(columns(by_att)):
        delta[n : n + 1, t * TILE : (t + 1) * TILE] = jnp.sum((column.astype(F32) * x1[at[n], :].astype(F32)).T, 0, keepdims=True)
        x4[at[n], :] = column


def attention_block(head, first, key, many, strips, edge, x1, x4, k, v, db, dq, lse, delta):
    kk, vv = k[rows(key, many), :], v[rows(key, many), :]
    at = [rows(head * TOKENS + first + s, STRIP) for s in strips]
    qs, dos = [x1[a, :] for a in at], [x4[a, :] for a in at]
    scores, dps = [dot_t(kk, q) for q in qs], [dot_t(vv, d) for d in dos]
    dk = dv = None
    for n, s in enumerate(strips):
        here = pl.ds(first + s, STRIP)
        p = jnp.exp2(scores[n] * E - lse[pl.ds(head, 1), here] * (E / SCALE))
        if edge and n == 0:
            shape = (STRIP, STRIP)
            p = jnp.where(lax.broadcasted_iota(jnp.int32, shape, 1) >= lax.broadcasted_iota(jnp.int32, shape, 0), p, 0.0)
        ds = (p * (dps[n] - delta[pl.ds(head, 1), here])).astype(BF)
        a, b = dot(p.astype(BF), dos[n]), dot(ds, qs[n])
        dv, dk = (a, b) if dv is None else (dv + a, dk + b)
        dq[:, s : s + STRIP] += dot(kk.T, ds)
    for base, part in ((0, dk), (TOKENS, dv)):
        db[pl.ds(pl.multiple_of(base + key, STRIP), many), :] += part


def turn_back(t, first, cos, sin):
    here = pl.ds(first, t.shape[0])
    t = t.astype(BF).astype(F32)
    return (t * cos[here, :] - pltpu.roll(t, HALF, 1) * sin[here, :]).astype(BF)


def backward_kernel(x_hbm, dy_hbm, att_hbm, attt_hbm, q_hbm, k_hbm, v_hbm, at_hbm, lse_hbm, cos_hbm, sin_hbm, wg_hbm, wu_hbm, wd_hbm, wo_hbm,
                    gd_hbm, gg_hbm, gu_hbm, ga_hbm, sq_hbm,
                    x1, x2, x3, x4, db, ff, dgu, wg, wu, wd, g, k, v, lse, delta, cos, sin, wo, xs, hs, dq, squares, total, came,
                    sem_x, sem_w, sem_in, sem_t, sem_sq, *rest):
    me = lax.axis_index("dp")
    barrier(me)
    colours, at = [Colour(dims) for dims in COLOURS], 0
    for number, colour in enumerate(colours):
        many = len(colour.scratch())
        colour.bind(rest[at : at + many], g, number, me, (gd_hbm, gg_hbm, gu_hbm, ga_hbm))
        at += many

    def load(src, dst, sem):
        return pltpu.make_async_copy(src, dst, sem)

    dys = [load(dy_hbm.at[0, :, pl.ds(n * LANE, LANE)], x3.at[pl.ds(n * TOKENS, TOKENS)], sem_x.at[n]) for n in range(HEADS)]
    first = load(wo_hbm.at[0], wo, sem_x.at[HEADS])
    later = [load(src, dst, sem_in.at[n]) for n, (src, dst) in enumerate(((k_hbm, k), (v_hbm, v), (lse_hbm, lse), (cos_hbm, cos), (sin_hbm, sin)))]
    swaps = [load(src, dst, sem_x.at[n]) for n, (src, dst) in enumerate(((att_hbm, x1), (attt_hbm, x2), (q_hbm, x1), (at_hbm, x2)))]

    def weights(i):
        par, cols = lax.rem(i, 2), rows(i * STEP, STEP)
        return [load(src, dst.at[par], sem_w.at[par, n]) for n, (src, dst) in enumerate(
            ((wg_hbm.at[0, :, cols], wg), (wu_hbm.at[0, :, cols], wu), (wd_hbm.at[0, cols, :], wd)))]

    def tile(t, slot):
        here = rows(t * TILE, TILE)
        heads = [load(att_hbm.at[pl.ds(n * TOKENS + pl.multiple_of(t * TILE, TILE), TILE)], stage(dgu, slot, n), sem_t.at[slot, n]) for n in range(HEADS)]
        return heads + [load(x_hbm.at[0, here], xs.at[slot], sem_t.at[slot, HEADS])]

    for copies in ([first], tile(0, 0), dys, tile(1, 1), weights(0), later):
        start(copies)
    db[...] = jnp.zeros_like(db)
    squares[...] = jnp.zeros_like(squares)
    for colour in colours:
        colour.zero()
    wait([first] + dys)

    def middle(n, _):
        for slot in range(2):
            t = 2 * n + slot
            wait(tile(t, slot))
            middle_tile(t, slot, x1, x2, x3, x4, dgu, xs, hs, wo)

            @pl.when(n == 0)
            def _():
                start(tile(t + 2, slot))

    lax.fori_loop(0, 2, middle, None)

    def body(i, _):
        par = lax.rem(i, 2)
        busy = (wg.at[par], wu.at[par], wd.at[par])

        def part(j):
            poll(colours, squares, i, j)

            @pl.when(i < MLP)
            def _():
                if j == 0:
                    wait(weights(i))

                    @pl.when(i + 1 < MLP)
                    def _():
                        start(weights(i + 1))

                if j < 2:
                    mlp_tile(j, x1, x3, *busy, ff, dgu)
                elif j == 2:
                    @pl.when(i == MLP - 1)
                    def _():
                        swaps[0].start()

                    def half(t, _):
                        add_input_gradient(t, busy[0], busy[1], dgu, db)
                    lax.fori_loop(0, 2, half, None)
                else:
                    slot = lax.rem(i, GS)
                    put(g, slot, 0, 0, dot(turned_block(x4), ff[...]))
                    put(g, slot, 1, 0, dot(turned_block(x2), dgu[:, :STEP]))
                    put(g, slot, 2, 0, dot(turned_block(x2), dgu[:, STEP:]))

            @pl.when(i == MLP)
            def _():
                if j == 0:
                    swaps[1].start()
                    swaps[0].wait()
                    wait(later)
                if j < 2:
                    for t in (2 * j, 2 * j + 1):
                        residual_tile(t, x1, x3, x4, db, hs, wo, delta)
                elif j == 2:
                    swaps[2].start()
                    swaps[1].wait()
                    db[: 2 * TOKENS, :] = jnp.zeros((2 * TOKENS, LANE), F32)
                if j >= 2:
                    def by_wo(n):
                        return dot(turned_block(x2), jnp.concatenate([x3[m * TOKENS : (m + 1) * TOKENS, :] for m in range(n, min(n + 2, HEADS))], 1))
                    for n in ((0, 2), (4, 6))[j - 2]:
                        put(g, (MLP + n // 6) % GS, (n // 2) % 3, 0, by_wo(n))
                if j == 3:
                    swaps[3].start()
                    swaps[2].wait()

            head = i - MLP - 1

            @pl.when((head >= 0) & (head < HEADS))
            def _():
                refs = (x1, x4, k, v, db, dq, lse, delta)
                late = WIDE if j in (1, 2) else 0
                if j < 2:
                    dq[...] = jnp.zeros_like(dq)
                if j == 1:
                    def seen(n, _):
                        attention_block(head, WIDE, n * TILE, TILE, range(0, WIDE, STRIP), False, *refs)
                    lax.fori_loop(0, 2, seen, None)
                if j in (0, 2):
                    for key in range(0, WIDE, STRIP):
                        attention_block(head, late, late + key, STRIP, range(key, WIDE, STRIP), True, *refs)
                    x3[rows(head * TOKENS + late, WIDE), :] = turn_back((dq[...] * SCALE).T, late, cos, sin)
                if j == 3:
                    @pl.when(head == 0)
                    def _():
                        swaps[3].wait()

                    def by_wq(n, many):
                        return dot(turned_block(x2), jnp.concatenate([x3[m * TOKENS : (m + 1) * TOKENS, :] for m in range(n, n + many)], 1))

                    for n in range(0, HEADS, 2):
                        @pl.when(head == n)
                        def _():
                            block = MLP + 1 + n // 6
                            if n == 0:
                                put(g, block % GS, 0, 1, by_wq(0, 1))
                            else:
                                put(g, block % GS, (n // 2) % 3, 0, by_wq(n - 1, 2))

            @pl.when(i == LAST)
            def _():
                if j == 3:
                    for n in range(2):
                        part = db[n * TOKENS : (n + 1) * TOKENS, :]
                        x1[n * TOKENS : (n + 1) * TOKENS, :] = part.astype(BF) if n else turn_back(part * SCALE, 0, cos, sin)
                    both = jnp.concatenate([x1[:TOKENS, :], x1[TOKENS : 2 * TOKENS, :]], 1)
                    put(g, (BLOCKS - 1) % GS, 1, 0, dot(turned_block(x2), both))

            if j == 0:
                for step in range(4):
                    @pl.when(i == SQUARES + step)
                    def _():
                        if step == 0:
                            wide = squares[0] + squares[1] + squares[2]
                            total[...] = wide[:8, :] + wide[8:, :]
                        exchange(step, total, came, sem_sq, me)

        for j in range(PER):
            part(j)
        return None

    lax.fori_loop(0, ROUNDS, body, None)
    copy = load(total, sq_hbm, sem_in.at[0])
    copy.start()
    copy.wait()


def backward(args):
    flat = pltpu.VMEM((FLAT, LANE), BF)
    narrow = pltpu.VMEM((TOKENS, LANE), BF)
    table, heads = pltpu.VMEM((TOKENS, LANE), F32), pltpu.VMEM((HEADS, TOKENS), F32)
    sem = pltpu.SemaphoreType.DMA
    thirds = len(COLOURS)
    return pl.pallas_call(
        backward_kernel,
        in_specs=[ANY] * len(args),
        out_specs=[ANY] * 5,
        out_shape=[like(MLP, 2, D, LANE), like(D, FF), like(D, FF), like(D, 6 * thirds * LANE), like(8, LANE, dtype=F32)],
        scratch_shapes=[flat] * 4
        + [pltpu.VMEM((FLAT, LANE), F32), pltpu.VMEM((TOKENS, STEP), BF), pltpu.VMEM((TOKENS, 2 * STEP), BF)]
        + [pltpu.VMEM((2, D, STEP), BF)] * 2
        + [pltpu.VMEM((2, STEP, D), BF), pltpu.VMEM((GS, thirds, ROWS, LANE), BF), narrow, narrow, heads, heads, table, table]
        + [pltpu.VMEM((D, D), BF), pltpu.VMEM((2, TILE, D), BF), pltpu.VMEM((TOKENS, D), BF), pltpu.VMEM((LANE, WIDE), F32)]
        + [pltpu.VMEM((thirds, 16, LANE), F32), pltpu.VMEM((8, LANE), F32), pltpu.VMEM((thirds, 8, 8, LANE), F32)]
        + [sem((HEADS + 1,)), sem((2, thirds)), sem((5,)), sem((2, HEADS + 1)), sem((2, thirds, 8))]
        + [s for dims in COLOURS for s in Colour(dims).scratch()],
        compiler_params=pltpu.CompilerParams(collective_id=0, has_side_effects=True, vmem_limit_bytes=63 * MIB),
        cost_estimate=cost(16 * TOKENS * D * FF, 120),
    )(*args)


def adamw(w, m, v, new_w, new_m, new_v, g):
    m = 0.9 * m[0] + 0.1 * g
    v = 0.95 * v[0] + 0.05 * g * g
    wide = w[0].astype(F32)
    new_w[0] = (wide - 0.02 * (m * lax.rsqrt(v + 1e-8) + 0.1 * wide)).astype(BF)
    new_m[0], new_v[0] = m, v


def update_kernel(count, sq_ref, *refs):
    total = jnp.sum(jnp.sum(sq_ref[...], 0, keepdims=True), 1, keepdims=True)
    factor = jnp.minimum(1.0, 0.5 * lax.rsqrt(total / count + 1e-30))
    names = len(refs) // 7
    for k, ref in enumerate(refs[:names]):
        g = ref[...] if len(ref.shape) == 2 else jnp.concatenate([ref[0, half].T for half in range(2)])
        adamw(*refs[names + k :: names], g.astype(F32) * factor)


def update(steps, gs, gradients, blocks, sq, arrays, count):
    return pl.pallas_call(
        functools.partial(update_kernel, count),
        grid=(steps,),
        in_specs=[whole((8, LANE))] + gradients + blocks * 3,
        out_specs=blocks * 3,
        out_shape=[like(*a.shape, dtype=a.dtype) for a in arrays],
        compiler_params=ROOM,
    )(sq, *gs, *arrays)


IN_MLP, IN_ATTENTION = ("w_down", "w_gate", "w_up"), ("wo", "wq", "wk", "wv")
STEPS_REST = 4
REST = D // STEPS_REST


def down(shape):
    return pl.BlockSpec((1, *shape), lambda i: (0, i, 0))


def across(shape, col=None):
    return pl.BlockSpec(shape, (lambda i: (0,) * (len(shape) - 1) + (i,)) if col is None else lambda i: (i, col))


NAMES = ("wq", "wk", "wv", "wo", "w_gate", "w_up", "w_down")


def solution(mesh):
    def step(x, dy, *arrays):
        kinds = [dict(zip(NAMES, arrays[n : n + len(NAMES)])) for n in range(0, len(arrays), len(NAMES))]
        w = kinds[0]
        cos, sin = tables()
        q, k, v, at = project(x, w["wq"], w["wk"], w["wv"], cos, sin)
        att, attt, lse = attend(q, k, v)
        flat = lambda a: a.reshape(FLAT, LANE)
        *gs, sq = backward((x, dy, flat(att), flat(attt), flat(q), k, v, flat(at), lse, cos, sin, w["w_gate"], w["w_up"], w["w_down"], w["wo"]))
        count, new = sum(a.size for a in w.values()), {}
        third = across((D, STEP))
        for names, *rest in (
            (IN_MLP, MLP, gs[:3], [pl.BlockSpec((1, 2, D, LANE), lambda i: (i, 0, 0, 0)), third, third],
             [down((STEP, D))] + [across((1, D, STEP))] * 2),
            (IN_ATTENTION, STEPS_REST, gs[3:] * 4, [across((REST, D), n) for n in range(2)] + [across((REST, LANE), n) for n in (2 * HEADS, 2 * HEADS + 1)],
             [down((REST, D))] * 2 + [down((REST, LANE))] * 2),
        ):
            done = update(*rest, sq, [kind[name] for kind in kinds for name in names], count)
            new.update(zip([(n, name) for n in range(len(kinds)) for name in names], done))
        return tuple(new[n, name] for n in range(len(kinds)) for name in NAMES)

    states, all_of, ours = P(("rep", "dp"), None, None), P(None, None, None), P("rep", None, None)
    many = 3 * len(NAMES)
    return jax.shard_map(step, mesh=mesh, in_specs=(states, states) + (all_of,) * many, out_specs=(ours,) * many, check_vma=False)
```
